32 devices in a mesh: gx: 4 (over y, x), gy: 8 (over z, core).
Axes of the slice: x: 2, y: 2, z: 4, core: 2. Of those that a mesh axis runs over, the one named last changes fastest.
Arguments:
- u_wind: float32 [64, 64, 1024], P(None, 'gx', 'gy'), may hold values from -6 to 6
- v_wind: float32 [64, 64, 1024], P(None, 'gx', 'gy'), may hold values from -6 to 6
- w_wind: float32 [64, 64, 1024], P(None, 'gx', 'gy'), may hold values from -4 to 4
- pressure: float32 [64, 64, 1024], P(None, 'gx', 'gy'), may hold values from -6 to 6
- terrain_level: int32 [64, 1024], P('gx', 'gy'), may hold values from 0 to 8
- zone_width: int32 [4], replicated, may hold values from 5 to 16
- stiffness: float32 [64], replicated, may hold values from 0.25 to 2
- inflow_profile: float32 [2, 64], replicated, may hold values from -5 to 5
Outputs:
- u_final: float32 [64, 64, 1024], P(None, 'gx', 'gy')
- v_final: float32 [64, 64, 1024], P(None, 'gx', 'gy')
- w_final: float32 [64, 64, 1024], P(None, 'gx', 'gy')
- p_final: float32 [64, 64, 1024], P(None, 'gx', 'gy')
The draws below stay inside these ranges and needn't reach their ends.
Inputs may be any that keep to these rules, and one draw needn't show every extreme that they name: `zone_width`: zone widths in columns.
All inputs are finite; a program needn't handle non-finite values.
Results may differ from the reference program's by a relative error of at most 0.0001.
Values sent between devices are 32-bit elements; how exact they have to be, the bound alone decides.
A program may use at most 128 MiB of HBM per device.

```python
import math
import jax
import jax.numpy as jnp
from jax import lax

NZ = 64
SUB = 6
TERRAIN_MAX = 8
ZONE_MAX = 16
NX = 64
NY = 1024


def place_ends(values, rng, least, largest):
    dims = values.shape
    index_at = [jax.random.randint(jax.random.fold_in(rng, axis), (), 0, dims[axis]) for axis in range(len(dims))]
    values = values.at[tuple(index_at)].set(least)
    longest = dims.index(max(dims))
    index_at[longest] = (index_at[longest] + 1) % dims[longest]
    return values.at[tuple(index_at)].set(largest)


def block_scale(key, shape, split, smallest, high):
    gain = 1.0
    for dim, shards_of in split:
        heights = jax.random.uniform(jax.random.fold_in(jax.random.fold_in(key, 6), dim), (shards_of,), jnp.float32, smallest / len(split), high / len(split))
        gain = gain * jnp.repeat(jnp.exp(heights), shape[dim] // shards_of).reshape((-1,) + (1,) * (len(shape) - 1 - dim))
    return gain


def centred(rng, shape, spread, most, split=(), held_as=jnp.bfloat16):
    drawn = jax.random.normal(rng, shape, jnp.float32) * spread
    if len(split) > 0:
        drawn = block_scale(rng, shape, split, -0.22, 0.18) * drawn
    return jnp.clip(drawn, min=-most, max=most).astype(held_as)


def setup_inputs(seed: int = 0) -> dict:
    seeds = jax.random.split(jax.random.key(seed), 9)
    u_wind = centred(seeds[0], (NZ, NX, NY), 1.0, 6.0, ((1, 4), (2, 8)), jnp.float32)
    v_wind = centred(seeds[1], (NZ, NX, NY), 1.0, 6.0, ((1, 4), (2, 8)), jnp.float32)
    w_wind = centred(seeds[2], (NZ, NX, NY), 0.5, 4.0, ((1, 4), (2, 8)), jnp.float32)
    pressure = centred(seeds[3], (NZ, NX, NY), 1.0, 6.0, ((1, 4), (2, 8)), jnp.float32)
    terrain_level = place_ends(jax.random.randint(seeds[4], (NX, NY), 0, TERRAIN_MAX + 1), jax.random.fold_in(seeds[4], 1), 0, TERRAIN_MAX).astype(jnp.int32)
    zone_width = place_ends(jax.random.randint(seeds[5], (4,), ZONE_MAX // 4 + 1, ZONE_MAX + 1), jax.random.fold_in(seeds[5], 1), ZONE_MAX // 4 + 1, ZONE_MAX).astype(jnp.int32)
    stiffness = jnp.clip(jnp.exp(jax.random.uniform(seeds[6], (NZ,), jnp.float32, math.log(0.25), math.log(2.0))), 0.25, 2.0)
    inflow_profile = centred(seeds[7], (2, NZ), 1.0, 5.0, (), jnp.float32)
    return dict(u_wind=u_wind, v_wind=v_wind, w_wind=w_wind, pressure=pressure, terrain_level=terrain_level, zone_width=zone_width, stiffness=stiffness, inflow_profile=inflow_profile)


ADV_COURANT = 0.3
H_COURANT = 0.4
Z_COURANT = 1.0
RELAX_STRENGTH = 0.5


def face_flux(scalar, velocity, along):
    extent = scalar.shape[along]
    count = extent - 5

    def offset(start):
        return lax.slice_in_dim(scalar, start, start + count, axis=along)

    centered = (37.0 * (offset(3) + offset(2)) - 8.0 * (offset(4) + offset(1)) + (offset(5) + offset(0))) / 60.0
    upwind = (10.0 * (offset(3) - offset(2)) - 5.0 * (offset(4) - offset(1)) + (offset(5) - offset(0))) / 60.0
    face_speed = lax.slice_in_dim(velocity, 3, 3 + count, axis=along)
    flux = face_speed * centered - jnp.abs(face_speed) * upwind
    return lax.slice_in_dim(flux, 1, count, axis=along) - lax.slice_in_dim(flux, 0, count - 1, axis=along)


def advect(extended, wet_inner):
    west_east = extended[0]
    south_north = extended[1]
    first = west_east.shape[1]
    second = west_east.shape[2]
    results = []
    for scalar in extended:
        tend_x = face_flux(scalar, west_east, 1)[:, :, 3:second - 3]
        tend_y = face_flux(scalar, south_north, 2)[:, 3:first - 3, :]
        inner = scalar[:, 3:first - 3, 3:second - 3]
        results.append(wet_inner * (inner - ADV_COURANT * (tend_x + tend_y)))
    return results


def relax_plane(col_index, row_index, x_total, y_total, zones):
    zone_f = zones.astype(jnp.float32)
    west_ramp = jnp.maximum(zone_f[0] - col_index, 0.0) / zone_f[0]
    east_ramp = jnp.maximum(zone_f[1] - (x_total - 1.0 - col_index), 0.0) / zone_f[1]
    south_ramp = jnp.maximum(zone_f[2] - row_index, 0.0) / zone_f[2]
    north_ramp = jnp.maximum(zone_f[3] - (y_total - 1.0 - row_index), 0.0) / zone_f[3]
    along_x = jnp.maximum(west_ramp, east_ramp)[:, None]
    along_y = jnp.maximum(south_ramp, north_ramp)[None, :]
    return RELAX_STRENGTH * jnp.maximum(along_x, along_y)


def thomas(sub_diag, main_diag, super_diag, right_side):
    def eliminate(carry, row):
        c_prev, d_prev = carry
        low_row, main_row, up_row, rhs_row = row
        pivot_value = main_row - low_row * c_prev
        c_new = up_row / pivot_value
        d_new = (rhs_row - low_row * d_prev) / pivot_value
        return (c_new, d_new), (c_new, d_new)

    zero_plane = jnp.zeros_like(main_diag[0])
    unused, (c_all, d_all) = lax.scan(eliminate, (zero_plane, zero_plane), (sub_diag, main_diag, super_diag, right_side), unroll=8)

    def substitute(x_next, row):
        c_row, d_row = row
        value = d_row - c_row * x_next
        return value, value

    unused_last, solved = lax.scan(substitute, zero_plane, (c_all, d_all), reverse=True, unroll=8)
    return solved


def shift_down(field):
    return jnp.concatenate([jnp.zeros_like(field[:1]), field[:-1]], axis=0)


def shift_up(field):
    return jnp.concatenate([field[1:], jnp.zeros_like(field[:1])], axis=0)


def column_solve(w_wind, q_field, wet_mask, g_level):
    factor = Z_COURANT * Z_COURANT
    g_cell = g_level * wet_mask
    g_above = shift_up(g_cell)
    wet_below = shift_down(wet_mask)
    sub_diag = -factor * g_cell * wet_below
    super_diag = -factor * g_above * wet_mask
    main_diag = 1.0 + wet_mask * factor * (g_above + g_cell)
    right_side = wet_mask * (w_wind - Z_COURANT * (shift_up(q_field) - q_field))
    return thomas(sub_diag, main_diag, super_diag, right_side)


def local_west(field):
    return jnp.concatenate([jnp.zeros_like(field[:, :1, :]), field[:, :-1, :]], axis=1)


def local_east(field):
    return jnp.concatenate([field[:, 1:, :], jnp.zeros_like(field[:, :1, :])], axis=1)


def local_south(field):
    return jnp.concatenate([jnp.zeros_like(field[:, :, :1]), field[:, :, :-1]], axis=2)


def local_north(field):
    return jnp.concatenate([field[:, :, 1:], jnp.zeros_like(field[:, :, :1])], axis=2)


def substep_update(carried, wet_mask, relax, g_level, u_bound, v_bound, from_west, from_south, from_east, from_north):
    u_wind, v_wind, w_wind, pressure = carried
    u_wind = wet_mask * (u_wind - H_COURANT * (pressure - from_west(pressure)))
    v_wind = wet_mask * (v_wind - H_COURANT * (pressure - from_south(pressure)))
    divergence = H_COURANT * (from_east(u_wind) - u_wind + from_north(v_wind) - v_wind)
    q_field = wet_mask * (pressure - g_level * divergence)
    w_wind = column_solve(w_wind, q_field, wet_mask, g_level)
    pressure = wet_mask * (q_field - g_level * Z_COURANT * (w_wind - shift_down(w_wind)))
    u_wind = u_wind - relax * (u_wind - wet_mask * u_bound)
    v_wind = v_wind - relax * (v_wind - wet_mask * v_bound)
    w_wind = w_wind - relax * w_wind
    pressure = pressure - relax * pressure
    return (u_wind, v_wind, w_wind, pressure)


def reference(u_wind, v_wind, w_wind, pressure, terrain_level, zone_width, stiffness, inflow_profile):
    levels = jnp.arange(NZ).astype(jnp.float32)[:, None, None]
    wet_mask = (levels >= terrain_level.astype(jnp.float32)[None, :, :]).astype(jnp.float32)
    padding = ((0, 0), (3, 3), (3, 3))
    extended = [jnp.pad(field, padding) for field in (u_wind, v_wind, w_wind, pressure)]
    carried = tuple(advect(extended, wet_mask))
    col_index = jnp.arange(NX).astype(jnp.float32)
    row_index = jnp.arange(NY).astype(jnp.float32)
    relax = relax_plane(col_index, row_index, float(NX), float(NY), zone_width)
    g_level = stiffness[:, None, None]
    u_bound = inflow_profile[0][:, None, None]
    v_bound = inflow_profile[1][:, None, None]
    for substep in range(SUB):
        carried = substep_update(carried, wet_mask, relax, g_level, u_bound, v_bound, local_west, local_south, local_east, local_north)
    return carried[0], carried[1], carried[2], carried[3]
```

```python
import functools

import jax
import jax.numpy as jnp
from jax import lax
from jax.experimental import pallas as pl
from jax.experimental.pallas import tpu as pltpu
from jax.sharding import PartitionSpec as P

SUB = 6
ADV = 0.3
HC = 0.4
ZC = 1.0
RELAX = 0.5
TERRAIN_MAX = 8
DRY = 1 << 20
WEST, EAST, SOUTH, NORTH = 0, 1, 2, 3
FU, FP, FV, FW = 0, 1, 2, 3
LO = 8
ROWS = 40
PEXT = 32
GROUP = 16
HALF = 32
CENT = {-3: 1.0, -2: -8.0, -1: 37.0, 0: 37.0, 1: -8.0, 2: 1.0}
UPW = {-3: -1.0, -2: 5.0, -1: -10.0, 0: 10.0, 1: -5.0, 2: 1.0}


def stencil(c, m3, m2, m1, f0, e1, e2):
    centered = 37.0 * (f0 + m1) - 8.0 * (e1 + m2) + (e2 + m3)
    upwind = 10.0 * (f0 - m1) - 5.0 * (e1 - m2) + (e2 - m3)
    return c * centered - jnp.abs(c) * upwind


def weights(dist, table):
    out = jnp.zeros(dist.shape, jnp.float32)
    for off, value in table.items():
        out = jnp.where(dist == off, value, out)
    return out.astype(jnp.bfloat16)


def split(x):
    hi = x.astype(jnp.bfloat16)
    return hi, (x - hi.astype(jnp.float32)).astype(jnp.bfloat16)


def kernel(
    nz,
    bx,
    cnt,
    u_in,
    v_in,
    w_in,
    p_in,
    terr,
    zone,
    g,
    prof,
    u_out,
    v_out,
    w_out,
    p_out,
    raw,
    tend,
    pres,
    wsc,
    q_buf,
    d_buf,
    cc,
    li,
    wi,
    lhs,
    mat,
    mat_c,
    prod,
    c_next,
    ys,
    yr,
    trx,
    tr_y,
    pw_r,
    pe_r,
    ps_y,
    pr_y,
    uh_x,
    vs_y,
    vr_y,
    ub_x,
    gh_x,
    wet_x,
    in_s,
    ini_s,
    ini_r,
    iny_s,
    iny_r,
    ter_s,
    ter_r,
    uv_s,
    uv_r,
    stp_s,
    stp_r,
):
    by = 128
    nkg = nz // GROUP
    nh = nz // HALF
    gx = lax.axis_index("gx")
    gy = lax.axis_index("gy")
    nx_dev, ny_dev = cnt
    has = (gx > 0, gx < nx_dev - 1, gy > 0, gy < ny_dev - 1)
    peer = ({"gx": gx - 1}, {"gx": gx + 1}, {"gy": gy - 1}, {"gy": gy + 1})
    opp = (EAST, WEST, NORTH, SOUTH)

    loads = [
        pltpu.make_async_copy(src, raw.at[f, :, pl.ds(LO, bx), :], in_s.at[f])
        for f, src in ((FU, u_in), (FP, p_in), (FV, v_in), (FW, w_in))
    ]
    for c in loads:
        c.start()

    barrier = pltpu.get_barrier_semaphore()
    for d in range(4):

        @pl.when(has[d])
        def _(d=d):
            pl.semaphore_signal(
                barrier, inc=1, device_id=peer[d], device_id_type=pl.DeviceIdType.MESH
            )

    def rcopy(d, src, dst, ss, rs):
        return pltpu.make_async_remote_copy(
            src_ref=src,
            dst_ref=dst,
            send_sem=ss,
            recv_sem=rs,
            device_id=peer[d],
            device_id_type=pl.DeviceIdType.MESH,
        )

    def start(d, *copies):
        @pl.when(has[d])
        def _():
            for c in copies:
                rcopy(d, *c).start()

    def wait_send(d, *copies):
        @pl.when(has[d])
        def _():
            for c in copies:
                rcopy(d, *c).wait_send()

    def wait_recv(d, *copies):
        @pl.when(has[opp[d]])
        def _():
            for c in copies:
                rcopy(d, *c).wait_recv()

    def ini(d, grp, c):
        out = []
        for r in range(3):
            own = LO + r if d == WEST else LO + bx - 3 + r
            far = LO + bx + r if d == WEST else LO - 3 + r
            f = pl.ds(2 * grp, 2)
            k = pl.ds(c * GROUP, GROUP)
            out.append(
                (
                    raw.at[f, k, own, :],
                    raw.at[f, k, far, :],
                    ini_s.at[d, grp, c, r],
                    ini_r.at[d, grp, c, r],
                )
            )
        return out

    def iny(d, c):
        return ys.at[c], yr.at[d - 2, c], iny_s.at[d - 2, c], iny_r.at[d - 2, c]

    def ter(d):
        if d == WEST:
            return terr.at[pl.ds(0, 8)], trx, ter_s.at[0], ter_r.at[0]
        return terr, tr_y, ter_s.at[1], ter_r.at[1]

    def uvx(h):
        k = pl.ds(h * HALF, HALF)
        return u_out.at[k, 0, :], uh_x.at[k], uv_s.at[h], uv_r.at[h]

    def uvy():
        return vs_y, vr_y, uv_s.at[nh], uv_r.at[nh]

    def stp(d, s, h=0):
        sems = stp_s.at[d, s, h], stp_r.at[d, s, h]
        if d < 2:
            k = pl.ds(h * HALF, HALF)
            row = LO if d == WEST else LO + bx - 1
            return pres.at[k, row, :], (pe_r, pw_r)[d].at[s, k], *sems
        return ps_y.at[s], pr_y.at[d - 2, s], *sems

    rows = lax.broadcasted_iota(jnp.int32, (bx, by), 0)
    lane = lax.broadcasted_iota(jnp.int32, (bx, by), 1)
    zero = jnp.zeros((bx, by), jnp.float32)

    def slab(k):
        return pl.ds(pl.multiple_of(k * bx, bx), bx)

    zrow = jnp.zeros((8, by), jnp.float32)

    def clear(k, carry):
        pres[k, pl.ds(0, 8), :] = zrow
        return carry

    lax.fori_loop(0, nz, clear, 0, unroll=8)

    for d in range(4):

        @pl.when(jnp.logical_not(has[opp[d]]))
        def _(d=d):
            if d == WEST:
                pe_r[...] = jnp.zeros(pe_r.shape, jnp.float32)
                uh_x[...] = jnp.zeros(uh_x.shape, jnp.float32)
                trx[...] = jnp.full(trx.shape, DRY, jnp.int32)
            if d == EAST:
                pw_r[...] = jnp.zeros(pw_r.shape, jnp.float32)
            if d < 2:
                at = pl.ds(LO + bx if d == WEST else 0, 8)

                def blank(k, carry):
                    for f in range(4):
                        raw[f, k, at, :] = zrow
                    return carry

                lax.fori_loop(0, nz, blank, 0, unroll=4)
            else:
                yr[d - 2] = jnp.zeros(yr.shape[1:], jnp.float32)
                pr_y[d - 2] = jnp.zeros(pr_y.shape[1:], jnp.float32)
            if d == SOUTH:
                tr_y[...] = jnp.full(tr_y.shape, DRY, jnp.int32)
                vr_y[...] = jnp.zeros(vr_y.shape, jnp.float32)

    loads[0].wait()
    loads[1].wait()
    pl.semaphore_wait(barrier, sum(h.astype(jnp.int32) for h in has))
    start(WEST, *[x for c in range(nkg) for x in ini(WEST, 0, c)])
    start(EAST, *[x for c in range(nkg) for x in ini(EAST, 0, c)])
    start(WEST, ter(WEST))
    start(SOUTH, ter(SOUTH))
    loads[2].wait()
    loads[3].wait()
    start(WEST, *[x for c in range(nkg) for x in ini(WEST, 1, c)])
    start(EAST, *[x for c in range(nkg) for x in ini(EAST, 1, c)])

    def pack(kg, carry):
        for f in range(4):
            acc = zero
            for kk in range(GROUP):
                x = raw[f, kg * GROUP + kk, pl.ds(LO, bx), :]
                acc = jnp.where((lane >> 3) == kk, pltpu.roll(x, 8 * kk + 3, 1), acc)
            ys[kg, f] = acc
        start(SOUTH, iny(SOUTH, kg))
        start(NORTH, iny(NORTH, kg))
        return carry

    lax.fori_loop(0, nkg, pack, 0)

    sq_r = lax.broadcasted_iota(jnp.int32, (by, by), 0)
    sq_c = lax.broadcasted_iota(jnp.int32, (by, by), 1)
    part = sq_r & 7
    far = jnp.where(part < 3, part - 3, jnp.where(part < 6, by - 3 + part, 8 * by))
    for src, at in ((sq_r, 0), (far, 2 * by)):
        for n in range(4):
            w = weights(src - sq_c - n // 2, (CENT, UPW)[n % 2])
            mat[pl.ds(at, by), pl.ds(n * by, by)] = w
            mat[pl.ds(at + by, by), pl.ds(n * by, by)] = w
        w = weights(src - sq_c - 1, {0: 1.0})
        mat_c[pl.ds(at, by), :] = w
        mat_c[pl.ds(at + by, by), :] = w

    def relax_of(ci, rj):
        best = None
        for n, dist in enumerate(
            (ci, (nx_dev * bx - 1.0) - ci, rj, (ny_dev * by - 1.0) - rj)
        ):
            width = jnp.full(ci.shape, zone[n], jnp.int32).astype(jnp.float32)
            ramp = jnp.maximum(width - dist, 0.0) / width
            best = ramp if best is None else jnp.maximum(best, ramp)
        return RELAX * best

    start_x = gx * bx
    start_y = gy * by
    ci = (rows + start_x).astype(jnp.float32)
    rj = (lane + start_y).astype(jnp.float32)
    relax = relax_of(ci, rj)
    keep = 1.0 - relax
    relax_hx = relax_of(
        (jnp.zeros((8, by), jnp.int32) + (start_x + bx)).astype(jnp.float32), rj[:8]
    )
    relax_hy = relax_of(ci, (jnp.zeros((bx, by), jnp.int32) + (start_y + by)).astype(jnp.float32))

    t0 = terr[...]

    def coeff(k, carry):
        c_prev, vrow = carry
        wet = t0 <= k
        gk = (ZC * ZC) * g[k]
        ga = (ZC * ZC) * jnp.where(k + 1 < nz, g[jnp.minimum(k + 1, nz - 1)], 0.0)
        inv = jnp.where(wet, 1.0 / (1.0 + ((ga + gk) - gk * c_prev)), 0.0)
        c_new = ga * inv
        wi[slab(k), :] = inv
        li[slab(k), :] = gk * inv
        cc[slab(k), :] = c_new
        ub_x[pl.ds(k, 1), :] = jnp.full((1, by), prof[0, k], jnp.float32)
        gh_x[pl.ds(k, 1), :] = jnp.full((1, by), g[k] * (HC * HC), jnp.float32)
        vrow = jnp.where((lane >> 1) == k, prof[1, k], vrow)
        return c_new, vrow

    _, vb_y = lax.fori_loop(0, nz, coeff, (zero, zero))

    wait_recv(WEST, ter(WEST))
    wait_recv(SOUTH, ter(SOUTH))
    sub8 = lax.broadcasted_iota(jnp.int32, (8, by), 0)
    t_east = jnp.broadcast_to(trx[0:1, :], (8, by))
    for k in range(0, nz, 8):
        wet_x[pl.ds(k, 8), :] = jnp.where(t_east <= sub8 + k, 1.0, 0.0)
    t_north = jnp.broadcast_to(tr_y[:, 0:1], (bx, by))
    wet_y = jnp.where(t_north <= (lane >> 1), 1.0, 0.0)

    scale = ADV / 60.0

    def along_y(kg, carry):
        wait_recv(SOUTH, iny(SOUTH, kg))
        wait_recv(NORTH, iny(NORTH, kg))
        for f in (FV, FU, FP, FW):
            halo = split(
                jnp.where((lane & 7) < 3, yr[NORTH - 2, kg, f], yr[SOUTH - 2, kg, f])
            )
            for kk in range(GROUP):
                at = pl.ds(kk * bx, bx)
                hi, lo = split(raw[f, kg * GROUP + kk, pl.ds(LO, bx), :])
                lhs[at, pl.ds(0, by)] = hi
                lhs[at, pl.ds(by, by)] = lo
                mine = (lane >> 3) == kk
                for n in range(2):
                    lhs[at, pl.ds((2 + n) * by, by)] = jnp.where(mine, halo[n], 0.0).astype(
                        jnp.bfloat16
                    )
            if f == FV:
                c_next[...] = scale * jnp.dot(
                    lhs[...], mat_c[...], preferred_element_type=jnp.float32
                )
            prod[...] = jnp.dot(lhs[...], mat[...], preferred_element_type=jnp.float32)
            for kk in range(GROUP):
                at = pl.ds(kk * bx, bx)
                k = kg * GROUP + kk
                c0 = raw[FV, k, pl.ds(LO, bx), :] * scale
                c1 = c_next[at, :]
                low = c0 * prod[at, pl.ds(0, by)] - jnp.abs(c0) * prod[at, pl.ds(by, by)]
                high = c1 * prod[at, pl.ds(2 * by, by)] - jnp.abs(c1) * prod[at, pl.ds(3 * by, by)]
                tend[f, slab(k), :] = raw[f, k, pl.ds(LO, bx), :] - (high - low)
        return carry

    lax.fori_loop(0, nkg, along_y, 0)

    def along_x(k, fields):
        n = bx + 8
        c = raw[FU, k, pl.ds(LO, n), :] * scale
        wet = t0 <= k
        res = []
        for f in fields:
            sh = [raw[f, k, pl.ds(LO + o, n), :] for o in (-3, -2, -1, 0, 1, 2)]
            flux = stencil(c, *sh)
            nxt = pltpu.roll(flux, n - 1, 0)[:bx]
            res.append(jnp.where(wet, tend[f, slab(k), :] - (nxt - flux[:bx]), 0.0))
        return res

    def wait_ini(grp, c):
        for d in (WEST, EAST):
            wait_recv(d, *ini(d, grp, c))

    def first(k, acc):
        u, p = along_x(k, (FU, FP))
        p = HC * p
        u_out[k] = u
        pres[k, pl.ds(LO, bx), :] = p
        return jnp.where((lane >> 1) == k, pltpu.roll(p, 2 * k + 1, 1), acc)

    acc = zero
    for h in range(nh):
        for c in range(h * HALF // GROUP, (h + 1) * HALF // GROUP):
            wait_ini(0, c)
            acc = lax.fori_loop(c * GROUP, (c + 1) * GROUP, first, acc, unroll=4)
        start(WEST, uvx(h), stp(WEST, 0, h))
        start(EAST, stp(EAST, 0, h))
    ps_y[0] = acc
    start(SOUTH, stp(SOUTH, 0))
    start(NORTH, stp(NORTH, 0))

    def second(k, acc):
        v, w = along_x(k, (FV, FW))
        v_out[k] = v
        wsc[slab(k), :] = HC * w
        return jnp.where((lane >> 1) == k, pltpu.roll(v, 2 * k + 1, 1), acc)

    acc = zero
    for c in range(nkg):
        wait_ini(1, c)
        acc = lax.fori_loop(c * GROUP, (c + 1) * GROUP, second, acc, unroll=4)
    vs_y[...] = acc
    start(SOUTH, uvy())

    for d in (WEST, EAST):
        wait_send(d, *[x for grp in range(2) for c in range(nkg) for x in ini(d, grp, c)])
    for d in (SOUTH, NORTH):
        wait_send(d, *[iny(d, c) for c in range(nkg)])
    for d in (WEST, SOUTH):
        wait_send(d, ter(d))
    wait_send(WEST, *[uvx(h) for h in range(nh)])
    wait_send(SOUTH, uvy())
    wait_recv(WEST, *[uvx(h) for h in range(nh)])
    wait_recv(SOUTH, uvy())
    vh0 = pltpu.roll(vr_y[...], by - 1, 1)
    even = (lane & 1) == 0
    edge = jnp.logical_or(lane == 0, lane == by - 1)
    keep_w = jnp.broadcast_to(keep[0:1], (8, by))
    wet_lo = jnp.broadcast_to(t0[0:1], (8, by)) <= sub8
    wet_hi = jnp.broadcast_to(t0[bx - 1 : bx], (8, by)) <= sub8

    def inner(k0, n, masked):
        stores = []
        for i in range(n):
            k = k0 + i
            p0 = pres[k, pl.ds(LO, bx), :]
            pm = pres[k, pl.ds(LO - 1, bx), :]
            un = u_out[k] - (p0 - pm)
            vn = v_out[k] - (p0 - jnp.where(lane == 0, 0.0, pltpu.roll(p0, 1, 1)))
            if masked:
                wet = t0 <= k
                un = jnp.where(wet, un, 0.0)
                vn = jnp.where(wet, vn, 0.0)
            un1 = jnp.where(rows == bx - 1, 0.0, pltpu.roll(un, bx - 1, 0))
            vn1 = jnp.where(lane == by - 1, 0.0, pltpu.roll(vn, by - 1, 1))
            q = p0 - (g[k] * (HC * HC)) * ((un1 - un) + (vn1 - vn))
            ur = keep * un + relax * prof[0, k]
            vr = keep * vn + relax * prof[1, k]
            if masked:
                q = jnp.where(wet, q, 0.0)
                ur = jnp.where(wet, ur, 0.0)
                vr = jnp.where(wet, vr, 0.0)
            stores.append((k, q, ur, vr))
        for k, q, ur, vr in stores:
            q_buf[slab(k), :] = q
            u_out[k] = ur
            v_out[k] = vr

    def edges_y(k0, n, halo, masked):
        stores = []
        for i in range(n):
            k = k0 + i
            add = jnp.where(edge, pltpu.roll(halo, by - 1 - 2 * k, 1), 0.0)
            if masked:
                add = jnp.where(t0 <= k, add, 0.0)
            q = q_buf[slab(k), :] + (g[k] * (HC * HC)) * add
            v = v_out[k] + jnp.where(lane == 0, keep * add, 0.0)
            stores.append((k, q, v))
        for k, q, v in stores:
            q_buf[slab(k), :] = q
            v_out[k] = v

    wide = 8

    def over(body, *args):
        body(0, TERRAIN_MAX, *args, True)

        def step(n, carry):
            body(TERRAIN_MAX + n * wide, wide, *args, False)
            return carry

        lax.fori_loop(0, (nz - TERRAIN_MAX) // wide, step, 0)

    def substep(s, vh):
        over(inner)

        wait_recv(SOUTH, stp(SOUTH, s))
        wait_recv(NORTH, stp(NORTH, s))
        vn_h = wet_y * (vh - (pltpu.roll(pr_y[SOUTH - 2, s], by - 1, 1) - ps_y[s]))
        vh_next = vn_h - relax_hy * (vn_h - wet_y * vb_y)
        halo = jnp.where(even, -vn_h, pltpu.roll(pr_y[NORTH - 2, s], 1, 1))
        over(edges_y, halo)

        for d in (WEST, EAST):
            wait_recv(d, *[stp(d, s, h) for h in range(nh)])
        for n in range(0, nz, 8):
            at = pl.ds(n, 8)
            gh = gh_x[at, :]
            pw = pw_r[s, at, :]
            if n < TERRAIN_MAX:
                pw = jnp.where(wet_lo, pw, 0.0)
            first_row = pl.ds(n * bx, 8, stride=bx)
            last_row = pl.ds(n * bx + bx - 1, 8, stride=bx)
            q_buf[first_row, :] = q_buf[first_row, :] + gh * pw
            u_out[pl.ds(n, 8), 0, :] = u_out[pl.ds(n, 8), 0, :] + keep_w * pw
            wet = wet_x[at, :]
            un = wet * (uh_x[at, :] - (pe_r[s, at, :] - pres[pl.ds(n, 8), LO + bx - 1, :]))
            uh_x[at, :] = un - relax_hx * (un - wet * ub_x[at, :])
            if n < TERRAIN_MAX:
                un = jnp.where(wet_hi, un, 0.0)
            q_buf[last_row, :] = q_buf[last_row, :] - gh * un

        q_prev = q_buf[slab(0), :]
        x = zero
        for k in range(nz):
            at = slab(k)
            q = q_buf[slab(k + 1), :] if k < nz - 1 else zero
            x = wi[at, :] * (wsc[at, :] - ZC * (q - q_prev)) + li[at, :] * x
            if k < nz - 1:
                d_buf[at, :] = x
            q_prev = q

        for d in (WEST, EAST):
            wait_send(d, *[stp(d, s, h) for h in range(nh)])

        for h in range(nh - 1, -1, -1):
            for k in range((h + 1) * HALF - 1, h * HALF - 1, -1):
                below = zero
                if k > 0:
                    below = d_buf[slab(k - 1), :] + cc[slab(k - 1), :] * x
                pres[k, pl.ds(LO, bx), :] = (q_buf[slab(k), :] - (g[k] * ZC) * (x - below)) * keep
                wsc[slab(k), :] = x * keep
                x = below

            @pl.when(s < SUB - 1)
            def _(h=h):
                start(WEST, stp(WEST, s + 1, h))
                start(EAST, stp(EAST, s + 1, h))

        for d in (SOUTH, NORTH):
            wait_send(d, stp(d, s))

        @pl.when(s < SUB - 1)
        def _():
            acc = zero
            for k in range(nz):
                x = pltpu.roll(pres[k, pl.ds(LO, bx), :], 2 * k + 1, 1)
                acc = jnp.where((lane >> 1) == k, x, acc)
            ps_y[s + 1] = acc
            start(SOUTH, stp(SOUTH, s + 1))
            start(NORTH, stp(NORTH, s + 1))

        return vh_next

    lax.fori_loop(0, SUB, substep, vh0)

    def finish(k, carry):
        w_out[k] = wsc[slab(k), :] * (1.0 / HC)
        p_out[k] = pres[k, pl.ds(LO, bx), :] * (1.0 / HC)
        return carry

    lax.fori_loop(0, nz, finish, 0, unroll=4)


def solution(mesh):
    cnt = (mesh.shape["gx"], mesh.shape["gy"])

    def on_device(u, v, w, p, terr, zone, g, prof):
        nz, bx, by = u.shape
        assert by == 128 and bx == 16 and 2 * nz == by and nz % HALF == 0
        f32 = jnp.float32
        vm = pltpu.VMEM
        dma = pltpu.SemaphoreType.DMA
        nkg = nz // GROUP
        nh = nz // HALF
        lev = vm((nz * bx, by), f32)
        col = vm((nz, by), f32)
        plane = vm((bx, by), f32)
        scratch = [
            vm((4, nz, ROWS, by), f32),
            vm((4, nz * bx, by), f32),
            vm((nz, PEXT, by), f32),
            lev, lev, lev, lev, lev, lev,
            vm((GROUP * bx, 4 * by), jnp.bfloat16),
            vm((4 * by, 4 * by), jnp.bfloat16),
            vm((4 * by, by), jnp.bfloat16),
            vm((GROUP * bx, 4 * by), f32),
            vm((GROUP * bx, by), f32),
            vm((nkg, 4, bx, by), f32),
            vm((2, nkg, 4, bx, by), f32),
            vm((8, by), jnp.int32),
            vm((bx, by), jnp.int32),
            vm((SUB, nz, by), f32),
            vm((SUB, nz, by), f32),
            vm((SUB, bx, by), f32),
            vm((2, SUB, bx, by), f32),
            col, plane, plane, col, col, col,
            dma((4,)),
            dma((2, 2, nkg, 3)), dma((2, 2, nkg, 3)),
            dma((2, nkg)), dma((2, nkg)),
            dma((2,)), dma((2,)),
            dma((nh + 1,)), dma((nh + 1,)),
            dma((4, SUB, nh)), dma((4, SUB, nh)),
        ]
        vspec = pl.BlockSpec(memory_space=pltpu.VMEM)
        sspec = pl.BlockSpec(memory_space=pltpu.SMEM)
        aspec = pl.BlockSpec(memory_space=pl.ANY)
        return pl.pallas_call(
            functools.partial(kernel, nz, bx, cnt),
            out_shape=[pltpu.VMEM((nz, bx, by), f32)] * 4,
            in_specs=[aspec] * 4 + [vspec] + [sspec] * 3,
            out_specs=[vspec] * 4,
            scratch_shapes=scratch,
            compiler_params=pltpu.CompilerParams(collective_id=0, has_side_effects=True),
        )(u, v, w, p, terr, zone, g, prof)

    field = P(None, "gx", "gy")
    return jax.shard_map(
        on_device,
        mesh=mesh,
        in_specs=(field, field, field, field, P("gx", "gy"), P(), P(), P()),
        out_specs=(field,) * 4,
        check_vma=False,
    )
```

```python
import functools

import jax
import jax.numpy as jnp
from jax import lax
from jax.experimental import pallas as pl
from jax.experimental.pallas import tpu as pltpu
from jax.sharding import PartitionSpec as P

SUB = 6
ADV = 0.3
HC = 0.4
ZC = 1.0
RELAX = 0.5
TERRAIN_MAX = 8
DRY = 1 << 20
WEST, EAST, SOUTH, NORTH = 0, 1, 2, 3
FU, FP, FV, FW = 0, 1, 2, 3
LO = 8
ROWS = 40
PEXT = 32
GROUP = 16
HALF = 32
CENT = {-3: 1.0, -2: -8.0, -1: 37.0, 0: 37.0, 1: -8.0, 2: 1.0}
UPW = {-3: -1.0, -2: 5.0, -1: -10.0, 0: 10.0, 1: -5.0, 2: 1.0}


def stencil(c, m3, m2, m1, f0, e1, e2):
    centered = 37.0 * (f0 + m1) - 8.0 * (e1 + m2) + (e2 + m3)
    upwind = 10.0 * (f0 - m1) - 5.0 * (e1 - m2) + (e2 - m3)
    return c * centered - jnp.abs(c) * upwind


def weights(dist, table):
    out = jnp.zeros(dist.shape, jnp.float32)
    for off, value in table.items():
        out = jnp.where(dist == off, value, out)
    return out.astype(jnp.bfloat16)


def split(x):
    hi = x.astype(jnp.bfloat16)
    return hi, (x - hi.astype(jnp.float32)).astype(jnp.bfloat16)


def kernel(
    nz,
    bx,
    cnt,
    u_in,
    v_in,
    w_in,
    p_in,
    terr_in,
    zone_in,
    g_in,
    prof_in,
    u_out,
    v_out,
    w_out,
    p_out,
    terr,
    zone,
    g,
    prof,
    raw,
    tend,
    pres,
    wsc,
    q_buf,
    d_buf,
    cc,
    li,
    wi,
    lhs,
    mat,
    mat_c,
    prod,
    c_next,
    ys,
    yr,
    trx,
    tr_y,
    pw_r,
    pe_r,
    ps_y,
    pr_y,
    uh_x,
    vs_y,
    vr_y,
    ub_x,
    gh_x,
    wet_x,
    in_s,
    ini_s,
    ini_r,
    iny_s,
    iny_r,
    ter_s,
    ter_r,
    uv_s,
    uv_r,
    stp_s,
    stp_r,
    hop,
    hop_s,
    hop_r,
    fwd_s,
):
    by = 128
    nkg = nz // GROUP
    nh = nz // HALF
    gx = lax.axis_index("gx")
    gy = lax.axis_index("gy")
    nx_dev, ny_dev = cnt
    has = (gx > 0, gx < nx_dev - 1, gy > 0, gy < ny_dev - 1)
    peer = ({"gx": gx - 1}, {"gx": gx + 1}, {"gy": gy - 1}, {"gy": gy + 1})
    opp = (EAST, WEST, NORTH, SOUTH)

    relay = nx_dev == 4
    inner_x = jnp.logical_or(gx == 1, gx == 2)

    barrier = pltpu.get_barrier_semaphore()

    def greet(dev):
        pl.semaphore_signal(barrier, inc=1, device_id=dev, device_id_type=pl.DeviceIdType.MESH)

    for d in range(4):

        @pl.when(has[d])
        def _(d=d):
            greet(peer[d])

    if relay:
        greet({"gx": lax.rem(gx + 2, 4)})

    loads = [
        pltpu.make_async_copy(src, raw.at[f, :, pl.ds(LO, bx), :], in_s.at[f])
        for f, src in ((FU, u_in), (FP, p_in), (FV, v_in), (FW, w_in))
    ]
    small = [
        pltpu.make_async_copy(src, dst, in_s.at[4 + n])
        for n, (src, dst) in enumerate(
            ((terr_in, terr), (zone_in, zone), (g_in, g), (prof_in, prof))
        )
    ]
    for c in loads + small:
        c.start()

    def rcopy(d, src, dst, ss, rs):
        return pltpu.make_async_remote_copy(
            src_ref=src,
            dst_ref=dst,
            send_sem=ss,
            recv_sem=rs,
            device_id=peer[d],
            device_id_type=pl.DeviceIdType.MESH,
        )

    def start(d, *copies):
        @pl.when(has[d])
        def _():
            for c in copies:
                rcopy(d, *c).start()

    def wait_send(d, *copies):
        @pl.when(has[d])
        def _():
            for c in copies:
                rcopy(d, *c).wait_send()

    def wait_recv(d, *copies):
        @pl.when(has[opp[d]])
        def _():
            for c in copies:
                rcopy(d, *c).wait_recv()

    def ini(d, grp, c):
        out = []
        for r in range(3):
            own = LO + r if d == WEST else LO + bx - 3 + r
            far = LO + bx + r if d == WEST else LO - 3 + r
            f = pl.ds(2 * grp, 2)
            k = pl.ds(c * GROUP, GROUP)
            out.append(
                (
                    raw.at[f, k, own, :],
                    raw.at[f, k, far, :],
                    ini_s.at[d, grp, c, r],
                    ini_r.at[d, grp, c, r],
                )
            )
        return out

    def direct(d):
        if not relay:
            return has[d]
        return jnp.logical_and(has[d], gx != (2, 1)[d])

    def rcopy_to(dev, src, dst, ss, rs):
        return pltpu.make_async_remote_copy(
            src_ref=src,
            dst_ref=dst,
            send_sem=ss,
            recv_sem=rs,
            device_id={"gx": dev},
            device_id_type=pl.DeviceIdType.MESH,
        )

    def to_relay(d, c):
        return [
            (x[0], hop.at[c, r], hop_s.at[c, r], hop_r.at[c, r])
            for r, x in enumerate(ini(d, 1, c))
        ]

    def from_relay(d, c):
        return [
            (hop.at[c, r], x[1], fwd_s.at[c, r], x[3]) for r, x in enumerate(ini(d, 1, c))
        ]

    def iny(d, c):
        return ys.at[c], yr.at[d - 2, c], iny_s.at[d - 2, c], iny_r.at[d - 2, c]

    def ter(d):
        if d == WEST:
            return terr.at[pl.ds(0, 8)], trx, ter_s.at[0], ter_r.at[0]
        return terr, tr_y, ter_s.at[1], ter_r.at[1]

    def uvx(h):
        k = pl.ds(h * HALF, HALF)
        return u_out.at[k, 0, :], uh_x.at[k], uv_s.at[h], uv_r.at[h]

    def uvy():
        return vs_y, vr_y, uv_s.at[nh], uv_r.at[nh]

    def stp(d, s, h=0):
        sems = stp_s.at[d, s, h], stp_r.at[d, s, h]
        if d < 2:
            k = pl.ds(h * HALF, HALF)
            row = LO if d == WEST else LO + bx - 1
            return pres.at[k, row, :], (pe_r, pw_r)[d].at[s, k], *sems
        return ps_y.at[s], pr_y.at[d - 2, s], *sems

    rows = lax.broadcasted_iota(jnp.int32, (bx, by), 0)
    lane = lax.broadcasted_iota(jnp.int32, (bx, by), 1)
    zero = jnp.zeros((bx, by), jnp.float32)

    def slab(k):
        return pl.ds(pl.multiple_of(k * bx, bx), bx)

    zrow = jnp.zeros((8, by), jnp.float32)

    def clear(k, carry):
        pres[k, pl.ds(0, 8), :] = zrow
        return carry

    lax.fori_loop(0, nz, clear, 0, unroll=8)

    for d in range(4):

        @pl.when(jnp.logical_not(has[opp[d]]))
        def _(d=d):
            if d == WEST:
                pe_r[...] = jnp.zeros(pe_r.shape, jnp.float32)
                uh_x[...] = jnp.zeros(uh_x.shape, jnp.float32)
                trx[...] = jnp.full(trx.shape, DRY, jnp.int32)
            if d == EAST:
                pw_r[...] = jnp.zeros(pw_r.shape, jnp.float32)
            if d < 2:
                at = pl.ds(LO + bx if d == WEST else 0, 8)

                def blank(k, carry):
                    for f in range(4):
                        raw[f, k, at, :] = zrow
                    return carry

                lax.fori_loop(0, nz, blank, 0, unroll=4)
            else:
                yr[d - 2] = jnp.zeros(yr.shape[1:], jnp.float32)
                pr_y[d - 2] = jnp.zeros(pr_y.shape[1:], jnp.float32)
            if d == SOUTH:
                tr_y[...] = jnp.full(tr_y.shape, DRY, jnp.int32)
                vr_y[...] = jnp.zeros(vr_y.shape, jnp.float32)

    small[0].wait()
    loads[0].wait()
    loads[1].wait()
    pl.semaphore_wait(barrier, sum(h.astype(jnp.int32) for h in has) + int(relay))
    start(WEST, ter(WEST))
    start(SOUTH, ter(SOUTH))
    start(WEST, *[x for c in range(nkg) for x in ini(WEST, 0, c)])
    start(EAST, *[x for c in range(nkg) for x in ini(EAST, 0, c)])
    loads[2].wait()
    loads[3].wait()
    if relay:
        for d, at in ((EAST, 1), (WEST, 2)):

            @pl.when(gx == at)
            def _(d=d):
                for c in range(nkg):
                    for x in to_relay(d, c):
                        rcopy_to(lax.rem(gx + 2, 4), *x).start()

    for d in (WEST, EAST):

        @pl.when(direct(d))
        def _(d=d):
            for c in range(nkg):
                for x in ini(d, 1, c):
                    rcopy(d, *x).start()

    for c in small[1:]:
        c.wait()

    def pack(kg, carry):
        for f in range(4):
            acc = zero
            for kk in range(GROUP):
                x = raw[f, kg * GROUP + kk, pl.ds(LO, bx), :]
                acc = jnp.where((lane >> 3) == kk, pltpu.roll(x, 8 * kk + 3, 1), acc)
            ys[kg, f] = acc
        start(SOUTH, iny(SOUTH, kg))
        start(NORTH, iny(NORTH, kg))
        return carry

    lax.fori_loop(0, nkg, pack, 0)

    sq_r = lax.broadcasted_iota(jnp.int32, (by, by), 0)
    sq_c = lax.broadcasted_iota(jnp.int32, (by, by), 1)
    part = sq_r & 7
    far = jnp.where(part < 3, part - 3, jnp.where(part < 6, by - 3 + part, 8 * by))
    for src, at in ((sq_r, 0), (far, 2 * by)):
        for n in range(4):
            w = weights(src - sq_c - n // 2, (CENT, UPW)[n % 2])
            mat[pl.ds(at, by), pl.ds(n * by, by)] = w
            mat[pl.ds(at + by, by), pl.ds(n * by, by)] = w
        w = weights(src - sq_c - 1, {0: 1.0})
        mat_c[pl.ds(at, by), :] = w
        mat_c[pl.ds(at + by, by), :] = w

    def relax_of(ci, rj):
        best = None
        for n, dist in enumerate(
            (ci, (nx_dev * bx - 1.0) - ci, rj, (ny_dev * by - 1.0) - rj)
        ):
            width = jnp.full(ci.shape, zone[n], jnp.int32).astype(jnp.float32)
            ramp = jnp.maximum(width - dist, 0.0) / width
            best = ramp if best is None else jnp.maximum(best, ramp)
        return RELAX * best

    start_x = gx * bx
    start_y = gy * by
    ci = (rows + start_x).astype(jnp.float32)
    rj = (lane + start_y).astype(jnp.float32)
    relax = relax_of(ci, rj)
    keep = 1.0 - relax
    relax_hx = relax_of(
        (jnp.zeros((8, by), jnp.int32) + (start_x + bx)).astype(jnp.float32), rj[:8]
    )
    relax_hy = relax_of(ci, (jnp.zeros((bx, by), jnp.int32) + (start_y + by)).astype(jnp.float32))

    t0 = terr[...]

    def coeff(k, carry):
        c_prev, vrow = carry
        wet = t0 <= k
        gk = (ZC * ZC) * g[k]
        ga = (ZC * ZC) * jnp.where(k + 1 < nz, g[jnp.minimum(k + 1, nz - 1)], 0.0)
        inv = jnp.where(wet, 1.0 / (1.0 + ((ga + gk) - gk * c_prev)), 0.0)
        c_new = ga * inv
        wi[slab(k), :] = inv
        li[slab(k), :] = gk * inv
        cc[slab(k), :] = c_new
        ub_x[pl.ds(k, 1), :] = jnp.full((1, by), prof[0, k], jnp.float32)
        gh_x[pl.ds(k, 1), :] = jnp.full((1, by), g[k] * (HC * HC), jnp.float32)
        vrow = jnp.where((lane >> 1) == k, prof[1, k], vrow)
        return c_new, vrow

    _, vb_y = lax.fori_loop(0, nz, coeff, (zero, zero))

    sub8 = lax.broadcasted_iota(jnp.int32, (8, by), 0)
    scale = ADV / 60.0

    def along_y(kg, carry):
        wait_recv(SOUTH, iny(SOUTH, kg))
        wait_recv(NORTH, iny(NORTH, kg))
        for f in (FV, FU, FP, FW):
            halo = split(
                jnp.where((lane & 7) < 3, yr[NORTH - 2, kg, f], yr[SOUTH - 2, kg, f])
            )
            for kk in range(GROUP):
                at = pl.ds(kk * bx, bx)
                hi, lo = split(raw[f, kg * GROUP + kk, pl.ds(LO, bx), :])
                lhs[at, pl.ds(0, by)] = hi
                lhs[at, pl.ds(by, by)] = lo
                mine = (lane >> 3) == kk
                for n in range(2):
                    lhs[at, pl.ds((2 + n) * by, by)] = jnp.where(mine, halo[n], 0.0).astype(
                        jnp.bfloat16
                    )
            if f == FV:
                c_next[...] = scale * jnp.dot(
                    lhs[...], mat_c[...], preferred_element_type=jnp.float32
                )
            prod[...] = jnp.dot(lhs[...], mat[...], preferred_element_type=jnp.float32)
            for kk in range(GROUP):
                at = pl.ds(kk * bx, bx)
                k = kg * GROUP + kk
                c0 = raw[FV, k, pl.ds(LO, bx), :] * scale
                c1 = c_next[at, :]
                low = c0 * prod[at, pl.ds(0, by)] - jnp.abs(c0) * prod[at, pl.ds(by, by)]
                high = c1 * prod[at, pl.ds(2 * by, by)] - jnp.abs(c1) * prod[at, pl.ds(3 * by, by)]
                tend[f, slab(k), :] = raw[f, k, pl.ds(LO, bx), :] - (high - low)
        return carry

    lax.fori_loop(0, nkg, along_y, 0)

    if relay:
        for d, at in ((EAST, 3), (WEST, 0)):

            @pl.when(gx == at)
            def _(d=d):
                for c in range(nkg):
                    for x, y in zip(to_relay(d, c), from_relay(d, c)):
                        rcopy_to(lax.rem(gx + 2, 4), *x).wait_recv()
                        rcopy_to((gx + 1, gx - 1)[d == EAST], *y).start()

    wait_recv(WEST, ter(WEST))
    wait_recv(SOUTH, ter(SOUTH))
    t_east = jnp.broadcast_to(trx[0:1, :], (8, by))
    for k in range(0, nz, 8):
        wet_x[pl.ds(k, 8), :] = jnp.where(t_east <= sub8 + k, 1.0, 0.0)
    t_north = jnp.broadcast_to(tr_y[:, 0:1], (bx, by))
    wet_y = jnp.where(t_north <= (lane >> 1), 1.0, 0.0)


    def along_x(k, fields):
        n = bx + 8
        c = raw[FU, k, pl.ds(LO, n), :] * scale
        wet = t0 <= k
        res = []
        for f in fields:
            sh = [raw[f, k, pl.ds(LO + o, n), :] for o in (-3, -2, -1, 0, 1, 2)]
            flux = stencil(c, *sh)
            nxt = pltpu.roll(flux, n - 1, 0)[:bx]
            res.append(jnp.where(wet, tend[f, slab(k), :] - (nxt - flux[:bx]), 0.0))
        return res

    def wait_ini(grp, c):
        for d in (WEST, EAST):
            wait_recv(d, *ini(d, grp, c))

    def first(k, acc):
        u, p = along_x(k, (FU, FP))
        p = HC * p
        u_out[k] = u
        pres[k, pl.ds(LO, bx), :] = p
        return jnp.where((lane >> 1) == k, pltpu.roll(p, 2 * k + 1, 1), acc)

    acc = zero
    for h in range(nh):
        for c in range(h * HALF // GROUP, (h + 1) * HALF // GROUP):
            wait_ini(0, c)
            acc = lax.fori_loop(c * GROUP, (c + 1) * GROUP, first, acc, unroll=4)
        start(WEST, uvx(h), stp(WEST, 0, h))
        start(EAST, stp(EAST, 0, h))
    ps_y[0] = acc
    start(SOUTH, stp(SOUTH, 0))
    start(NORTH, stp(NORTH, 0))

    def second(k, acc):
        v, w = along_x(k, (FV, FW))
        v_out[k] = v
        wsc[slab(k), :] = HC * w
        return jnp.where((lane >> 1) == k, pltpu.roll(v, 2 * k + 1, 1), acc)

    acc = zero
    for c in range(nkg):
        wait_ini(1, c)
        acc = lax.fori_loop(c * GROUP, (c + 1) * GROUP, second, acc, unroll=4)
    vs_y[...] = acc
    start(SOUTH, uvy())

    for d in (WEST, EAST):
        wait_send(d, *[x for c in range(nkg) for x in ini(d, 0, c)])

        @pl.when(direct(d))
        def _(d=d):
            for c in range(nkg):
                for x in ini(d, 1, c):
                    rcopy(d, *x).wait_send()

    if relay:

        @pl.when(inner_x)
        def _():
            for c in range(nkg):
                for x in to_relay(EAST, c):
                    rcopy_to(lax.rem(gx + 2, 4), *x).wait_send()

        @pl.when(jnp.logical_not(inner_x))
        def _():
            for c in range(nkg):
                for x in from_relay(EAST, c):
                    rcopy_to(lax.rem(gx + 2, 4), *x).wait_send()

    for d in (SOUTH, NORTH):
        wait_send(d, *[iny(d, c) for c in range(nkg)])
    for d in (WEST, SOUTH):
        wait_send(d, ter(d))
    wait_send(WEST, *[uvx(h) for h in range(nh)])
    wait_send(SOUTH, uvy())
    wait_recv(WEST, *[uvx(h) for h in range(nh)])
    wait_recv(SOUTH, uvy())
    vh0 = pltpu.roll(vr_y[...], by - 1, 1)
    even = (lane & 1) == 0
    edge = jnp.logical_or(lane == 0, lane == by - 1)
    keep_w = jnp.broadcast_to(keep[0:1], (8, by))
    wet_lo = jnp.broadcast_to(t0[0:1], (8, by)) <= sub8
    wet_hi = jnp.broadcast_to(t0[bx - 1 : bx], (8, by)) <= sub8

    def inner(k0, n, masked):
        stores = []
        for i in range(n):
            k = k0 + i
            p0 = pres[k, pl.ds(LO, bx), :]
            pm = pres[k, pl.ds(LO - 1, bx), :]
            un = u_out[k] - (p0 - pm)
            vn = v_out[k] - (p0 - jnp.where(lane == 0, 0.0, pltpu.roll(p0, 1, 1)))
            if masked:
                wet = t0 <= k
                un = jnp.where(wet, un, 0.0)
                vn = jnp.where(wet, vn, 0.0)
            un1 = jnp.where(rows == bx - 1, 0.0, pltpu.roll(un, bx - 1, 0))
            vn1 = jnp.where(lane == by - 1, 0.0, pltpu.roll(vn, by - 1, 1))
            q = p0 - (g[k] * (HC * HC)) * ((un1 - un) + (vn1 - vn))
            ur = keep * un + relax * prof[0, k]
            vr = keep * vn + relax * prof[1, k]
            if masked:
                q = jnp.where(wet, q, 0.0)
                ur = jnp.where(wet, ur, 0.0)
                vr = jnp.where(wet, vr, 0.0)
            stores.append((k, q, ur, vr))
        for k, q, ur, vr in stores:
            q_buf[slab(k), :] = q
            u_out[k] = ur
            v_out[k] = vr

    def edges_y(k0, n, halo, masked):
        stores = []
        for i in range(n):
            k = k0 + i
            add = jnp.where(edge, pltpu.roll(halo, by - 1 - 2 * k, 1), 0.0)
            if masked:
                add = jnp.where(t0 <= k, add, 0.0)
            q = q_buf[slab(k), :] + (g[k] * (HC * HC)) * add
            v = v_out[k] + jnp.where(lane == 0, keep * add, 0.0)
            stores.append((k, q, v))
        for k, q, v in stores:
            q_buf[slab(k), :] = q
            v_out[k] = v

    wide = 8

    def over(body, *args):
        body(0, TERRAIN_MAX, *args, True)

        def step(n, carry):
            body(TERRAIN_MAX + n * wide, wide, *args, False)
            return carry

        lax.fori_loop(0, (nz - TERRAIN_MAX) // wide, step, 0)

    def substep(s, vh):
        over(inner)

        wait_recv(SOUTH, stp(SOUTH, s))
        wait_recv(NORTH, stp(NORTH, s))
        vn_h = wet_y * (vh - (pltpu.roll(pr_y[SOUTH - 2, s], by - 1, 1) - ps_y[s]))
        vh_next = vn_h - relax_hy * (vn_h - wet_y * vb_y)
        halo = jnp.where(even, -vn_h, pltpu.roll(pr_y[NORTH - 2, s], 1, 1))
        over(edges_y, halo)

        for d in (WEST, EAST):
            wait_recv(d, *[stp(d, s, h) for h in range(nh)])
        for n in range(0, nz, 8):
            at = pl.ds(n, 8)
            gh = gh_x[at, :]
            pw = pw_r[s, at, :]
            if n < TERRAIN_MAX:
                pw = jnp.where(wet_lo, pw, 0.0)
            first_row = pl.ds(n * bx, 8, stride=bx)
            last_row = pl.ds(n * bx + bx - 1, 8, stride=bx)
            q_buf[first_row, :] = q_buf[first_row, :] + gh * pw
            u_out[pl.ds(n, 8), 0, :] = u_out[pl.ds(n, 8), 0, :] + keep_w * pw
            wet = wet_x[at, :]
            un = wet * (uh_x[at, :] - (pe_r[s, at, :] - pres[pl.ds(n, 8), LO + bx - 1, :]))
            uh_x[at, :] = un - relax_hx * (un - wet * ub_x[at, :])
            if n < TERRAIN_MAX:
                un = jnp.where(wet_hi, un, 0.0)
            q_buf[last_row, :] = q_buf[last_row, :] - gh * un

        q_prev = q_buf[slab(0), :]
        x = zero
        for k in range(nz):
            at = slab(k)
            q = q_buf[slab(k + 1), :] if k < nz - 1 else zero
            x = wi[at, :] * (wsc[at, :] - ZC * (q - q_prev)) + li[at, :] * x
            if k < nz - 1:
                d_buf[at, :] = x
            q_prev = q

        for d in (WEST, EAST):
            wait_send(d, *[stp(d, s, h) for h in range(nh)])

        for h in range(nh - 1, -1, -1):
            for k in range((h + 1) * HALF - 1, h * HALF - 1, -1):
                below = zero
                if k > 0:
                    below = d_buf[slab(k - 1), :] + cc[slab(k - 1), :] * x
                pres[k, pl.ds(LO, bx), :] = (q_buf[slab(k), :] - (g[k] * ZC) * (x - below)) * keep
                wsc[slab(k), :] = x * keep
                x = below

            @pl.when(s < SUB - 1)
            def _(h=h):
                start(WEST, stp(WEST, s + 1, h))
                start(EAST, stp(EAST, s + 1, h))

        for d in (SOUTH, NORTH):
            wait_send(d, stp(d, s))

        @pl.when(s < SUB - 1)
        def _():
            acc = zero
            for k in range(nz):
                x = pltpu.roll(pres[k, pl.ds(LO, bx), :], 2 * k + 1, 1)
                acc = jnp.where((lane >> 1) == k, x, acc)
            ps_y[s + 1] = acc
            start(SOUTH, stp(SOUTH, s + 1))
            start(NORTH, stp(NORTH, s + 1))

        return vh_next

    lax.fori_loop(0, SUB, substep, vh0)

    def finish(k, carry):
        w_out[k] = wsc[slab(k), :] * (1.0 / HC)
        p_out[k] = pres[k, pl.ds(LO, bx), :] * (1.0 / HC)
        return carry

    lax.fori_loop(0, nz, finish, 0, unroll=4)


def solution(mesh):
    cnt = (mesh.shape["gx"], mesh.shape["gy"])

    def on_device(u, v, w, p, terr, zone, g, prof):
        nz, bx, by = u.shape
        assert by == 128 and bx == 16 and 2 * nz == by and nz % HALF == 0
        f32 = jnp.float32
        vm = pltpu.VMEM
        dma = pltpu.SemaphoreType.DMA
        nkg = nz // GROUP
        nh = nz // HALF
        lev = vm((nz * bx, by), f32)
        col = vm((nz, by), f32)
        plane = vm((bx, by), f32)
        plane_i = vm((bx, by), jnp.int32)
        scratch = [
            plane_i,
            pltpu.SMEM(zone.shape, jnp.int32),
            pltpu.SMEM(g.shape, f32),
            pltpu.SMEM(prof.shape, f32),
            vm((4, nz, ROWS, by), f32),
            vm((4, nz * bx, by), f32),
            vm((nz, PEXT, by), f32),
            lev, lev, lev, lev, lev, lev,
            vm((GROUP * bx, 4 * by), jnp.bfloat16),
            vm((4 * by, 4 * by), jnp.bfloat16),
            vm((4 * by, by), jnp.bfloat16),
            vm((GROUP * bx, 4 * by), f32),
            vm((GROUP * bx, by), f32),
            vm((nkg, 4, bx, by), f32),
            vm((2, nkg, 4, bx, by), f32),
            vm((8, by), jnp.int32),
            vm((bx, by), jnp.int32),
            vm((SUB, nz, by), f32),
            vm((SUB, nz, by), f32),
            vm((SUB, bx, by), f32),
            vm((2, SUB, bx, by), f32),
            col, plane, plane, col, col, col,
            dma((8,)),
            dma((2, 2, nkg, 3)), dma((2, 2, nkg, 3)),
            dma((2, nkg)), dma((2, nkg)),
            dma((2,)), dma((2,)),
            dma((nh + 1,)), dma((nh + 1,)),
            dma((4, SUB, nh)), dma((4, SUB, nh)),
            vm((nkg, 3, 2, GROUP, by), f32),
            dma((nkg, 3)), dma((nkg, 3)), dma((nkg, 3)),
        ]
        vspec = pl.BlockSpec(memory_space=pltpu.VMEM)
        aspec = pl.BlockSpec(memory_space=pl.ANY)
        return pl.pallas_call(
            functools.partial(kernel, nz, bx, cnt),
            out_shape=[pltpu.VMEM((nz, bx, by), f32)] * 4,
            in_specs=[aspec] * 8,
            out_specs=[vspec] * 4,
            scratch_shapes=scratch,
            compiler_params=pltpu.CompilerParams(collective_id=0, has_side_effects=True),
        )(u, v, w, p, terr, zone, g, prof)

    field = P(None, "gx", "gy")
    return jax.shard_map(
        on_device,
        mesh=mesh,
        in_specs=(field, field, field, field, P("gx", "gy"), P(), P(), P()),
        out_specs=(field,) * 4,
        check_vma=False,
    )
```

```python
import functools

import jax
import jax.numpy as jnp
from jax import lax
from jax.experimental import pallas as pl
from jax.experimental.pallas import tpu as pltpu
from jax.sharding import PartitionSpec as P

SUB = 6
ADV = 0.3
HC = 0.4
ZC = 1.0
RELAX = 0.5
TERRAIN_MAX = 8
DRY = 1 << 20
WEST, EAST, SOUTH, NORTH = 0, 1, 2, 3
FU, FP, FV, FW = 0, 1, 2, 3
LO = 8
ROWS = 40
PEXT = 32
GROUP = 16
CENT = {-3: 1.0, -2: -8.0, -1: 37.0, 0: 37.0, 1: -8.0, 2: 1.0}
UPW = {-3: -1.0, -2: 5.0, -1: -10.0, 0: 10.0, 1: -5.0, 2: 1.0}


def stencil(c, m3, m2, m1, f0, e1, e2):
    centered = 37.0 * (f0 + m1) - 8.0 * (e1 + m2) + (e2 + m3)
    upwind = 10.0 * (f0 - m1) - 5.0 * (e1 - m2) + (e2 - m3)
    return c * centered - jnp.abs(c) * upwind


def weights(dist, table):
    out = jnp.zeros(dist.shape, jnp.float32)
    for off, value in table.items():
        out = jnp.where(dist == off, value, out)
    return out.astype(jnp.bfloat16)


def split(x):
    hi = x.astype(jnp.bfloat16)
    return hi, (x - hi.astype(jnp.float32)).astype(jnp.bfloat16)


def kernel(
    nz,
    bx,
    cnt,
    u_in,
    v_in,
    w_in,
    p_in,
    terr_in,
    zone_in,
    g_in,
    prof_in,
    u_out,
    v_out,
    w_out,
    p_out,
    terr,
    zone,
    g,
    prof,
    raw,
    tend,
    pres,
    wsc,
    q_buf,
    d_buf,
    cc,
    li,
    wi,
    lhs,
    mat,
    mat_c,
    prod,
    c_next,
    ys,
    yr,
    trx,
    tr_y,
    pw_r,
    pe_r,
    ps_y,
    pr_y,
    us_x,
    uh_x,
    vs_y,
    vr_y,
    ub_x,
    gh_x,
    wet_x,
    in_s,
    ini_s,
    ini_r,
    iny_s,
    iny_r,
    ter_s,
    ter_r,
    uv_s,
    uv_r,
    stp_s,
    stp_r,
    hop,
    hop_s,
    hop_r,
    fwd_s,
):
    by = 128
    nkg = nz // GROUP
    gx = lax.axis_index("gx")
    gy = lax.axis_index("gy")
    nx_dev, ny_dev = cnt
    has = (gx > 0, gx < nx_dev - 1, gy > 0, gy < ny_dev - 1)
    peer = ({"gx": gx - 1}, {"gx": gx + 1}, {"gy": gy - 1}, {"gy": gy + 1})
    opp = (EAST, WEST, NORTH, SOUTH)

    relay = nx_dev == 4
    inner_x = jnp.logical_or(gx == 1, gx == 2)

    barrier = pltpu.get_barrier_semaphore()

    def greet(dev):
        pl.semaphore_signal(barrier, inc=1, device_id=dev, device_id_type=pl.DeviceIdType.MESH)

    for d in range(4):

        @pl.when(has[d])
        def _(d=d):
            greet(peer[d])

    if relay:
        greet({"gx": lax.rem(gx + 2, 4)})

    loads = [
        pltpu.make_async_copy(src, raw.at[f, :, pl.ds(LO, bx), :], in_s.at[f])
        for f, src in ((FU, u_in), (FP, p_in), (FV, v_in), (FW, w_in))
    ]
    small = [
        pltpu.make_async_copy(src, dst, in_s.at[4 + n])
        for n, (src, dst) in enumerate(
            ((terr_in, terr), (zone_in, zone), (g_in, g), (prof_in, prof))
        )
    ]
    for c in loads + small:
        c.start()

    def rcopy(d, src, dst, ss, rs):
        return pltpu.make_async_remote_copy(
            src_ref=src,
            dst_ref=dst,
            send_sem=ss,
            recv_sem=rs,
            device_id=peer[d],
            device_id_type=pl.DeviceIdType.MESH,
        )

    def start(d, *copies):
        @pl.when(has[d])
        def _():
            for c in copies:
                rcopy(d, *c).start()

    def wait_send(d, *copies):
        @pl.when(has[d])
        def _():
            for c in copies:
                rcopy(d, *c).wait_send()

    def wait_recv(d, *copies):
        @pl.when(has[opp[d]])
        def _():
            for c in copies:
                rcopy(d, *c).wait_recv()

    def ini(d, grp, c=None):
        own = LO if d == WEST else LO + bx - 3
        far = LO + bx if d == WEST else LO - 3
        f = pl.ds(0, 2) if grp == 0 else grp + 1
        k = pl.ds(0, nz) if c is None else pl.ds(c * GROUP, GROUP)
        return (
            raw.at[f, k, pl.ds(own, 3), :],
            raw.at[f, k, pl.ds(far, 3), :],
            ini_s.at[d, grp],
            ini_r.at[d, grp, 0 if c is None else c],
        )

    def direct(d):
        if not relay:
            return has[d]
        return jnp.logical_and(has[d], gx != (2, 1)[d])

    def rcopy_to(dev, src, dst, ss, rs):
        return pltpu.make_async_remote_copy(
            src_ref=src,
            dst_ref=dst,
            send_sem=ss,
            recv_sem=rs,
            device_id={"gx": dev},
            device_id_type=pl.DeviceIdType.MESH,
        )

    def to_relay(d, grp):
        dst = hop.at[grp - 1, :, pl.ds(0, 3), :]
        return ini(d, grp)[0], dst, hop_s.at[grp - 1], hop_r.at[grp - 1]

    def from_relay(d, grp, c=None):
        k = pl.ds(0, nz) if c is None else pl.ds(c * GROUP, GROUP)
        _, dst, _, sem = ini(d, grp, c)
        return hop.at[grp - 1, k, pl.ds(0, 3), :], dst, fwd_s.at[grp - 1], sem

    def forward(grp):
        if relay:
            for d, at in ((EAST, 3), (WEST, 0)):

                @pl.when(gx == at)
                def _(d=d):
                    rcopy_to(lax.rem(gx + 2, 4), *to_relay(d, grp)).wait_recv()
                    for c in range(nkg):
                        rcopy_to((gx + 1, gx - 1)[d == EAST], *from_relay(d, grp, c)).start()

    def start_direct(grp):
        for d in (WEST, EAST):

            @pl.when(direct(d))
            def _(d=d):
                for c in range(nkg):
                    rcopy(d, *ini(d, grp, c)).start()

    def iny(d, c):
        return ys.at[c], yr.at[d - 2, c], iny_s.at[d - 2], iny_r.at[d - 2, c]

    def ter(d):
        if d == WEST:
            return terr.at[pl.ds(0, 8)], trx, ter_s.at[0], ter_r.at[0]
        return terr, tr_y, ter_s.at[1], ter_r.at[1]

    def uv(d):
        if d == WEST:
            return us_x, uh_x, uv_s.at[0], uv_r.at[0]
        return vs_y, vr_y, uv_s.at[1], uv_r.at[1]

    def stp(d, s):
        sems = stp_s.at[d], stp_r.at[d, lax.rem(s, 2)]
        if d < 2:
            row = LO if d == WEST else LO + bx - 1
            return pres.at[:, row, :], (pe_r, pw_r)[d].at[s], *sems
        return ps_y.at[s], pr_y.at[d - 2, s], *sems

    rows = lax.broadcasted_iota(jnp.int32, (bx, by), 0)
    lane = lax.broadcasted_iota(jnp.int32, (bx, by), 1)
    zero = jnp.zeros((bx, by), jnp.float32)

    def slab(k):
        return pl.ds(pl.multiple_of(k * bx, bx), bx)

    zrow = jnp.zeros((8, by), jnp.float32)

    def clear(k, carry):
        pres[k, pl.ds(0, 8), :] = zrow
        return carry

    lax.fori_loop(0, nz, clear, 0, unroll=8)

    for d in range(4):

        @pl.when(jnp.logical_not(has[opp[d]]))
        def _(d=d):
            if d == WEST:
                pe_r[...] = jnp.zeros(pe_r.shape, jnp.float32)
                uh_x[...] = jnp.zeros(uh_x.shape, jnp.float32)
                trx[...] = jnp.full(trx.shape, DRY, jnp.int32)
            if d == EAST:
                pw_r[...] = jnp.zeros(pw_r.shape, jnp.float32)
            if d < 2:
                at = pl.ds(LO + bx if d == WEST else 0, 8)

                def blank(k, carry):
                    for f in range(4):
                        raw[f, k, at, :] = zrow
                    return carry

                lax.fori_loop(0, nz, blank, 0, unroll=4)
            else:
                yr[d - 2] = jnp.zeros(yr.shape[1:], jnp.float32)
                pr_y[d - 2] = jnp.zeros(pr_y.shape[1:], jnp.float32)
            if d == SOUTH:
                tr_y[...] = jnp.full(tr_y.shape, DRY, jnp.int32)
                vr_y[...] = jnp.zeros(vr_y.shape, jnp.float32)

    small[0].wait()
    loads[0].wait()
    loads[1].wait()
    pl.semaphore_wait(barrier, sum(h.astype(jnp.int32) for h in has) + int(relay))
    start(WEST, ter(WEST))
    start(SOUTH, ter(SOUTH))
    for d in (WEST, EAST):
        start(d, *[ini(d, 0, c) for c in range(nkg)])
    loads[2].wait()
    loads[3].wait()
    if relay:
        for d, at in ((EAST, 1), (WEST, 2)):

            @pl.when(gx == at)
            def _(d=d):
                for grp in (1, 2):
                    rcopy_to(lax.rem(gx + 2, 4), *to_relay(d, grp)).start()

    start_direct(1)

    for c in small[1:]:
        c.wait()

    def pack(kg, carry):
        for f in range(4):
            acc = zero
            for kk in range(GROUP):
                x = raw[f, kg * GROUP + kk, pl.ds(LO, bx), :]
                acc = jnp.where((lane >> 3) == kk, pltpu.roll(x, 8 * kk + 3, 1), acc)
            ys[kg, f] = acc
        start(SOUTH, iny(SOUTH, kg))
        start(NORTH, iny(NORTH, kg))
        return carry

    lax.fori_loop(0, nkg, pack, 0)

    sq_r = lax.broadcasted_iota(jnp.int32, (by, by), 0)
    sq_c = lax.broadcasted_iota(jnp.int32, (by, by), 1)
    part = sq_r & 7
    far = jnp.where(part < 3, part - 3, jnp.where(part < 6, by - 3 + part, 8 * by))
    for src, at in ((sq_r, 0), (far, 2 * by)):
        for n in range(4):
            w = weights(src - sq_c - n // 2, (CENT, UPW)[n % 2])
            mat[pl.ds(at, by), pl.ds(n * by, by)] = w
            mat[pl.ds(at + by, by), pl.ds(n * by, by)] = w
        w = weights(src - sq_c - 1, {0: 1.0})
        mat_c[pl.ds(at, by), :] = w
        mat_c[pl.ds(at + by, by), :] = w

    def relax_of(ci, rj):
        best = None
        for n, dist in enumerate(
            (ci, (nx_dev * bx - 1.0) - ci, rj, (ny_dev * by - 1.0) - rj)
        ):
            width = jnp.full(ci.shape, zone[n], jnp.int32).astype(jnp.float32)
            ramp = jnp.maximum(width - dist, 0.0) / width
            best = ramp if best is None else jnp.maximum(best, ramp)
        return RELAX * best

    start_x = gx * bx
    start_y = gy * by
    ci = (rows + start_x).astype(jnp.float32)
    rj = (lane + start_y).astype(jnp.float32)
    relax = relax_of(ci, rj)
    keep = 1.0 - relax
    relax_hx = relax_of(
        (jnp.zeros((8, by), jnp.int32) + (start_x + bx)).astype(jnp.float32), rj[:8]
    )
    relax_hy = relax_of(ci, (jnp.zeros((bx, by), jnp.int32) + (start_y + by)).astype(jnp.float32))

    t0 = terr[...]

    def coeff(k, carry):
        c_prev, vrow = carry
        wet = t0 <= k
        gk = (ZC * ZC) * g[k]
        ga = (ZC * ZC) * jnp.where(k + 1 < nz, g[jnp.minimum(k + 1, nz - 1)], 0.0)
        inv = jnp.where(wet, 1.0 / (1.0 + ((ga + gk) - gk * c_prev)), 0.0)
        c_new = ga * inv
        wi[slab(k), :] = inv
        li[slab(k), :] = gk * inv
        cc[slab(k), :] = c_new
        ub_x[pl.ds(k, 1), :] = jnp.full((1, by), prof[0, k], jnp.float32)
        gh_x[pl.ds(k, 1), :] = jnp.full((1, by), g[k] * (HC * HC), jnp.float32)
        vrow = jnp.where((lane >> 1) == k, prof[1, k], vrow)
        return c_new, vrow

    _, vb_y = lax.fori_loop(0, nz, coeff, (zero, zero))

    sub8 = lax.broadcasted_iota(jnp.int32, (8, by), 0)
    scale = ADV / 60.0

    def along_y(kg, carry):
        wait_recv(SOUTH, iny(SOUTH, kg))
        wait_recv(NORTH, iny(NORTH, kg))
        for f in (FV, FU, FP, FW):
            halo = split(
                jnp.where((lane & 7) < 3, yr[NORTH - 2, kg, f], yr[SOUTH - 2, kg, f])
            )
            for kk in range(GROUP):
                at = pl.ds(kk * bx, bx)
                hi, lo = split(raw[f, kg * GROUP + kk, pl.ds(LO, bx), :])
                lhs[at, pl.ds(0, by)] = hi
                lhs[at, pl.ds(by, by)] = lo
                mine = (lane >> 3) == kk
                for n in range(2):
                    lhs[at, pl.ds((2 + n) * by, by)] = jnp.where(mine, halo[n], 0.0).astype(
                        jnp.bfloat16
                    )
            if f == FV:
                c_next[...] = scale * jnp.dot(
                    lhs[...], mat_c[...], preferred_element_type=jnp.float32
                )
            prod[...] = jnp.dot(lhs[...], mat[...], preferred_element_type=jnp.float32)
            for kk in range(GROUP):
                at = pl.ds(kk * bx, bx)
                k = kg * GROUP + kk
                c0 = raw[FV, k, pl.ds(LO, bx), :] * scale
                c1 = c_next[at, :]
                low = c0 * prod[at, pl.ds(0, by)] - jnp.abs(c0) * prod[at, pl.ds(by, by)]
                high = c1 * prod[at, pl.ds(2 * by, by)] - jnp.abs(c1) * prod[at, pl.ds(3 * by, by)]
                tend[f, slab(k), :] = raw[f, k, pl.ds(LO, bx), :] - (high - low)
        return carry

    lax.fori_loop(0, nkg, along_y, 0)

    forward(1)
    start_direct(2)

    wait_recv(WEST, ter(WEST))
    wait_recv(SOUTH, ter(SOUTH))
    t_east = jnp.broadcast_to(trx[0:1, :], (8, by))
    for k in range(0, nz, 8):
        wet_x[pl.ds(k, 8), :] = jnp.where(t_east <= sub8 + k, 1.0, 0.0)
    t_north = jnp.broadcast_to(tr_y[:, 0:1], (bx, by))
    wet_y = jnp.where(t_north <= (lane >> 1), 1.0, 0.0)


    def along_x(k, fields):
        n = bx + 8
        c = raw[FU, k, pl.ds(LO, n), :] * scale
        wet = t0 <= k
        res = []
        for f in fields:
            sh = [raw[f, k, pl.ds(LO + o, n), :] for o in (-3, -2, -1, 0, 1, 2)]
            flux = stencil(c, *sh)
            nxt = pltpu.roll(flux, n - 1, 0)[:bx]
            res.append(jnp.where(wet, tend[f, slab(k), :] - (nxt - flux[:bx]), 0.0))
        return res

    def wait_ini(grp, c):
        for d in (WEST, EAST):
            wait_recv(d, ini(d, grp, c))

    def first(k, acc):
        u, p = along_x(k, (FU, FP))
        p = HC * p
        u_out[k] = u
        pres[k, pl.ds(LO, bx), :] = p
        return jnp.where((lane >> 1) == k, pltpu.roll(p, 2 * k + 1, 1), acc)

    acc = zero
    for c in range(nkg):
        wait_ini(0, c)
        acc = lax.fori_loop(c * GROUP, (c + 1) * GROUP, first, acc, unroll=4)
    for n in range(0, nz, 8):
        us_x[pl.ds(n, 8), :] = u_out[pl.ds(n, 8), 0, :]
    start(WEST, stp(WEST, 0), uv(WEST))
    start(EAST, stp(EAST, 0))
    ps_y[0] = acc
    start(SOUTH, stp(SOUTH, 0))
    start(NORTH, stp(NORTH, 0))

    forward(2)

    def inner(k0, n, masked):
        stores = []
        for i in range(n):
            k = k0 + i
            p0 = pres[k, pl.ds(LO, bx), :]
            pm = pres[k, pl.ds(LO - 1, bx), :]
            un = u_out[k] - (p0 - pm)
            vn = v_out[k] - (p0 - jnp.where(lane == 0, 0.0, pltpu.roll(p0, 1, 1)))
            if masked:
                wet = t0 <= k
                un = jnp.where(wet, un, 0.0)
                vn = jnp.where(wet, vn, 0.0)
            un1 = jnp.where(rows == bx - 1, 0.0, pltpu.roll(un, bx - 1, 0))
            vn1 = jnp.where(lane == by - 1, 0.0, pltpu.roll(vn, by - 1, 1))
            q = p0 - (g[k] * (HC * HC)) * ((un1 - un) + (vn1 - vn))
            ur = keep * un + relax * prof[0, k]
            vr = keep * vn + relax * prof[1, k]
            if masked:
                q = jnp.where(wet, q, 0.0)
                ur = jnp.where(wet, ur, 0.0)
                vr = jnp.where(wet, vr, 0.0)
            stores.append((k, q, ur, vr))
        for k, q, ur, vr in stores:
            q_buf[slab(k), :] = q
            u_out[k] = ur
            v_out[k] = vr

    def second(k, acc):
        (v,) = along_x(k, (FV,))
        v_out[k] = v
        return jnp.where((lane >> 1) == k, pltpu.roll(v, 2 * k + 1, 1), acc)

    def third(k, carry):
        wsc[slab(k), :] = HC * along_x(k, (FW,))[0]
        return carry

    acc = zero
    for c in range(nkg):
        wait_ini(1, c)
        acc = lax.fori_loop(c * GROUP, (c + 1) * GROUP, second, acc, unroll=4)
        if c == 0:
            inner(0, TERRAIN_MAX, True)
            inner(TERRAIN_MAX, GROUP - TERRAIN_MAX, False)
        else:
            inner(c * GROUP, GROUP, False)
    vs_y[...] = acc
    start(SOUTH, uv(SOUTH))

    for c in range(nkg):
        wait_ini(2, c)
        lax.fori_loop(c * GROUP, (c + 1) * GROUP, third, 0, unroll=4)

    wait_recv(WEST, uv(WEST))
    wait_recv(SOUTH, uv(SOUTH))
    vh0 = pltpu.roll(vr_y[...], by - 1, 1)
    even = (lane & 1) == 0
    edge = jnp.logical_or(lane == 0, lane == by - 1)
    keep_w = jnp.broadcast_to(keep[0:1], (8, by))
    wet_lo = jnp.broadcast_to(t0[0:1], (8, by)) <= sub8
    wet_hi = jnp.broadcast_to(t0[bx - 1 : bx], (8, by)) <= sub8

    def edges_y(halo):
        for k in range(nz):
            add = jnp.where(edge, pltpu.roll(halo, by - 1 - 2 * k, 1), 0.0)
            if k < TERRAIN_MAX:
                add = jnp.where(t0 <= k, add, 0.0)
            q_buf[slab(k), :] = q_buf[slab(k), :] + (g[k] * (HC * HC)) * add
            v_out[k] = v_out[k] + jnp.where(lane == 0, keep * add, 0.0)

    wide = 8

    def over(body, *args):
        body(0, TERRAIN_MAX, *args, True)

        def step(n, carry):
            body(TERRAIN_MAX + n * wide, wide, *args, False)
            return carry

        lax.fori_loop(0, (nz - TERRAIN_MAX) // wide, step, 0)

    def substep(s, vh):
        wait_recv(SOUTH, stp(SOUTH, s))
        wait_recv(NORTH, stp(NORTH, s))
        vn_h = wet_y * (vh - (pltpu.roll(pr_y[SOUTH - 2, s], by - 1, 1) - ps_y[s]))
        vh_next = vn_h - relax_hy * (vn_h - wet_y * vb_y)
        halo = jnp.where(even, -vn_h, pltpu.roll(pr_y[NORTH - 2, s], 1, 1))
        edges_y(halo)

        for d in (WEST, EAST):
            wait_recv(d, stp(d, s))
        for n in range(0, nz, 8):
            at = pl.ds(n, 8)
            gh = gh_x[at, :]
            pw = pw_r[s, at, :]
            if n < TERRAIN_MAX:
                pw = jnp.where(wet_lo, pw, 0.0)
            first_row = pl.ds(n * bx, 8, stride=bx)
            last_row = pl.ds(n * bx + bx - 1, 8, stride=bx)
            q_buf[first_row, :] = q_buf[first_row, :] + gh * pw
            u_out[pl.ds(n, 8), 0, :] = u_out[pl.ds(n, 8), 0, :] + keep_w * pw
            wet = wet_x[at, :]
            un = wet * (uh_x[at, :] - (pe_r[s, at, :] - pres[pl.ds(n, 8), LO + bx - 1, :]))
            uh_x[at, :] = un - relax_hx * (un - wet * ub_x[at, :])
            if n < TERRAIN_MAX:
                un = jnp.where(wet_hi, un, 0.0)
            q_buf[last_row, :] = q_buf[last_row, :] - gh * un

        q_prev = q_buf[slab(0), :]
        x = zero
        for k in range(nz):
            at = slab(k)
            q = q_buf[slab(k + 1), :] if k < nz - 1 else zero
            x = wi[at, :] * (wsc[at, :] - ZC * (q - q_prev)) + li[at, :] * x
            if k < nz - 1:
                d_buf[at, :] = x
            q_prev = q

        for d in (WEST, EAST):
            wait_send(d, stp(d, s))

        for k in range(nz - 1, -1, -1):
            below = zero
            if k > 0:
                below = d_buf[slab(k - 1), :] + cc[slab(k - 1), :] * x
            pres[k, pl.ds(LO, bx), :] = (q_buf[slab(k), :] - (g[k] * ZC) * (x - below)) * keep
            wsc[slab(k), :] = x * keep
            x = below

        @pl.when(s < SUB - 1)
        def _():
            start(WEST, stp(WEST, s + 1))
            start(EAST, stp(EAST, s + 1))

        for d in (SOUTH, NORTH):
            wait_send(d, stp(d, s))

        @pl.when(s < SUB - 1)
        def _():
            acc = zero
            for k in range(nz):
                x = pltpu.roll(pres[k, pl.ds(LO, bx), :], 2 * k + 1, 1)
                acc = jnp.where((lane >> 1) == k, x, acc)
            ps_y[s + 1] = acc
            start(SOUTH, stp(SOUTH, s + 1))
            start(NORTH, stp(NORTH, s + 1))
            over(inner)

        return vh_next

    lax.fori_loop(0, SUB, substep, vh0)

    for d in (WEST, EAST):
        wait_send(d, ini(d, 0))

        @pl.when(direct(d))
        def _(d=d):
            for grp in (1, 2):
                rcopy(d, *ini(d, grp)).wait_send()

    if relay:

        @pl.when(inner_x)
        def _():
            for grp in (1, 2):
                rcopy_to(lax.rem(gx + 2, 4), *to_relay(EAST, grp)).wait_send()

        @pl.when(jnp.logical_not(inner_x))
        def _():
            for grp in (1, 2):
                rcopy_to(lax.rem(gx + 2, 4), *from_relay(EAST, grp)).wait_send()

    for d in (SOUTH, NORTH):
        wait_send(d, (ys, yr.at[d - 2], iny_s.at[d - 2], iny_r.at[d - 2, 0]))
    for d in (WEST, SOUTH):
        wait_send(d, ter(d), uv(d))

    def finish(k, carry):
        w_out[k] = wsc[slab(k), :] * (1.0 / HC)
        p_out[k] = pres[k, pl.ds(LO, bx), :] * (1.0 / HC)
        return carry

    lax.fori_loop(0, nz, finish, 0, unroll=4)


def emit(*refs):
    sems = refs[-1]
    copies = [pltpu.make_async_copy(refs[n], refs[4 + n], sems.at[n]) for n in range(4)]
    for c in copies:
        c.start()
    for c in copies:
        c.wait()


def solution(mesh):
    cnt = (mesh.shape["gx"], mesh.shape["gy"])

    def on_device(u, v, w, p, terr, zone, g, prof):
        nz, bx, by = u.shape
        assert by == 128 and bx == 16 and 2 * nz == by
        f32 = jnp.float32
        vm = pltpu.VMEM
        dma = pltpu.SemaphoreType.DMA
        nkg = nz // GROUP
        lev = vm((nz * bx, by), f32)
        col = vm((nz, by), f32)
        plane = vm((bx, by), f32)
        plane_i = vm((bx, by), jnp.int32)
        scratch = [
            plane_i,
            pltpu.SMEM(zone.shape, jnp.int32),
            pltpu.SMEM(g.shape, f32),
            pltpu.SMEM(prof.shape, f32),
            vm((4, nz, ROWS, by), f32),
            vm((4, nz * bx, by), f32),
            vm((nz, PEXT, by), f32),
            lev, lev, lev, lev, lev, lev,
            vm((GROUP * bx, 4 * by), jnp.bfloat16),
            vm((4 * by, 4 * by), jnp.bfloat16),
            vm((4 * by, by), jnp.bfloat16),
            vm((GROUP * bx, 4 * by), f32),
            vm((GROUP * bx, by), f32),
            vm((nkg, 4, bx, by), f32),
            vm((2, nkg, 4, bx, by), f32),
            vm((8, by), jnp.int32),
            vm((bx, by), jnp.int32),
            vm((SUB, nz, by), f32),
            vm((SUB, nz, by), f32),
            vm((SUB, bx, by), f32),
            vm((2, SUB, bx, by), f32),
            col, col, plane, plane, col, col, col,
            dma((8,)),
            dma((2, 3)), dma((2, 3, nkg)),
            dma((2,)), dma((2, nkg)),
            dma((2,)), dma((2,)),
            dma((2,)), dma((2,)),
            dma((4,)), dma((4, 2)),
            vm((2, nz, 8, by), f32),
            dma((2,)), dma((2,)), dma((2,)),
        ]
        vspec = pl.BlockSpec(memory_space=pltpu.VMEM)
        aspec = pl.BlockSpec(memory_space=pl.ANY)
        outs = pl.pallas_call(
            functools.partial(kernel, nz, bx, cnt),
            out_shape=[pltpu.VMEM((nz, bx, by), f32)] * 4,
            in_specs=[aspec] * 8,
            out_specs=[vspec] * 4,
            scratch_shapes=scratch,
            compiler_params=pltpu.CompilerParams(collective_id=0, has_side_effects=True),
        )(u, v, w, p, terr, zone, g, prof)
        outs = [pltpu.with_memory_space_constraint(a, pltpu.VMEM) for a in outs]
        return pl.pallas_call(
            emit,
            out_shape=[jax.ShapeDtypeStruct((nz, bx, by), f32)] * 4,
            in_specs=[vspec] * 4,
            out_specs=[aspec] * 4,
            scratch_shapes=[dma((4,))],
        )(*outs)

    field = P(None, "gx", "gy")
    return jax.shard_map(
        on_device,
        mesh=mesh,
        in_specs=(field, field, field, field, P("gx", "gy"), P(), P(), P()),
        out_specs=(field,) * 4,
        check_vma=False,
    )
```

```python
import functools

import jax
import jax.numpy as jnp
from jax import lax
from jax.experimental import pallas as pl
from jax.experimental.pallas import tpu as pltpu
from jax.sharding import PartitionSpec as P

SUB = 6
ADV = 0.3
HC = 0.4
ZC = 1.0
RELAX = 0.5
TERRAIN_MAX = 8
DRY = 1 << 20
WEST, EAST, SOUTH, NORTH = 0, 1, 2, 3
FU, FP, FV, FW = 0, 1, 2, 3
LO = 8
ROWS = 40
PEXT = 24
GROUP = 16
VMEM_LIMIT = 59 << 20
CENT = {-3: 1.0, -2: -8.0, -1: 37.0, 0: 37.0, 1: -8.0, 2: 1.0}
UPW = {-3: -1.0, -2: 5.0, -1: -10.0, 0: 10.0, 1: -5.0, 2: 1.0}


def stencil(c, m3, m2, m1, f0, e1, e2):
    centered = 37.0 * (f0 + m1) - 8.0 * (e1 + m2) + (e2 + m3)
    upwind = 10.0 * (f0 - m1) - 5.0 * (e1 - m2) + (e2 - m3)
    return c * centered - jnp.abs(c) * upwind


def weights(dist, table):
    out = jnp.zeros(dist.shape, jnp.float32)
    for off, value in table.items():
        out = jnp.where(dist == off, value, out)
    return out.astype(jnp.bfloat16)


def split(x):
    hi = x.astype(jnp.bfloat16)
    return hi, (x - hi.astype(jnp.float32)).astype(jnp.bfloat16)


def kernel(
    nz,
    bx,
    cnt,
    u_in,
    v_in,
    w_in,
    p_in,
    terr_in,
    zone_in,
    g_in,
    prof_in,
    u_out,
    v_out,
    wsc,
    q_buf,
    li,
    wi,
    cc,
    keep_out,
    gh_x,
    terr,
    zone,
    g,
    prof,
    raw,
    tend,
    pres,
    d_buf,
    lhs,
    mat,
    mat_c,
    prod,
    c_next,
    ys,
    yr,
    trx,
    tr_y,
    pw_r,
    pe_r,
    ps_y,
    pr_y,
    us_x,
    uh_x,
    vs_y,
    vr_y,
    ub_x,
    wet_x,
    in_s,
    ini_s,
    ini_r,
    iny_s,
    iny_r,
    ter_s,
    ter_r,
    uv_s,
    uv_r,
    stp_s,
    stp_r,
    hop,
    hop_r,
    fwd_s,
):
    by = 128
    nkg = nz // GROUP
    gx = lax.axis_index("gx")
    gy = lax.axis_index("gy")
    nx_dev, ny_dev = cnt
    has = (gx > 0, gx < nx_dev - 1, gy > 0, gy < ny_dev - 1)
    peer = ({"gx": gx - 1}, {"gx": gx + 1}, {"gy": gy - 1}, {"gy": gy + 1})
    opp = (EAST, WEST, NORTH, SOUTH)

    relay = nx_dev == 4
    inner_x = jnp.logical_or(gx == 1, gx == 2)

    barrier = pltpu.get_barrier_semaphore()

    def greet(dev):
        pl.semaphore_signal(barrier, inc=1, device_id=dev, device_id_type=pl.DeviceIdType.MESH)

    for d in range(4):

        @pl.when(has[d])
        def _(d=d):
            greet(peer[d])

    if relay:
        greet({"gx": lax.rem(gx + 2, 4)})

    loads = [
        pltpu.make_async_copy(src, raw.at[f, :, pl.ds(LO, bx), :], in_s.at[f])
        for f, src in ((FU, u_in), (FP, p_in), (FV, v_in), (FW, w_in))
    ]
    small = [
        pltpu.make_async_copy(src, dst, in_s.at[4 + n])
        for n, (src, dst) in enumerate(
            ((terr_in, terr), (zone_in, zone), (g_in, g), (prof_in, prof))
        )
    ]
    for c in loads + small:
        c.start()

    def rcopy(d, src, dst, ss, rs):
        return pltpu.make_async_remote_copy(
            src_ref=src,
            dst_ref=dst,
            send_sem=ss,
            recv_sem=rs,
            device_id=peer[d],
            device_id_type=pl.DeviceIdType.MESH,
        )

    def start(d, *copies):
        @pl.when(has[d])
        def _():
            for c in copies:
                rcopy(d, *c).start()

    def wait_send(d, *copies):
        @pl.when(has[d])
        def _():
            for c in copies:
                rcopy(d, *c).wait_send()

    def wait_recv(d, *copies):
        @pl.when(has[opp[d]])
        def _():
            for c in copies:
                rcopy(d, *c).wait_recv()

    def ini(d, grp, c=None):
        own = LO if d == WEST else LO + bx - 3
        far = LO + bx if d == WEST else LO - 3
        f = pl.ds(0, 2) if grp == 0 else grp + 1
        k = pl.ds(0, nz) if c is None else pl.ds(c * GROUP, GROUP)
        return (
            raw.at[f, k, pl.ds(own, 3), :],
            raw.at[f, k, pl.ds(far, 3), :],
            ini_s.at[d],
            ini_r.at[d, grp, 0 if c is None else c],
        )

    def direct(d):
        if not relay:
            return has[d]
        return jnp.logical_and(has[d], gx != (2, 1)[d])

    def rcopy_to(dev, src, dst, ss, rs):
        return pltpu.make_async_remote_copy(
            src_ref=src,
            dst_ref=dst,
            send_sem=ss,
            recv_sem=rs,
            device_id={"gx": dev},
            device_id_type=pl.DeviceIdType.MESH,
        )

    def to_relay(d, grp):
        dst = hop.at[grp - 1, :, pl.ds(0, 3), :]
        return ini(d, grp)[0], dst, ini_s.at[d], hop_r.at[grp - 1]

    def from_relay(d, grp, c=None):
        k = pl.ds(0, nz) if c is None else pl.ds(c * GROUP, GROUP)
        _, dst, _, sem = ini(d, grp, c)
        return hop.at[grp - 1, k, pl.ds(0, 3), :], dst, fwd_s.at[0], sem

    def forward(grp):
        if relay:
            for d, at in ((EAST, 3), (WEST, 0)):

                @pl.when(gx == at)
                def _(d=d):
                    rcopy_to(lax.rem(gx + 2, 4), *to_relay(d, grp)).wait_recv()
                    for c in range(nkg):
                        rcopy_to((gx + 1, gx - 1)[d == EAST], *from_relay(d, grp, c)).start()

    def start_direct(grp):
        for d in (WEST, EAST):

            @pl.when(direct(d))
            def _(d=d):
                for c in range(nkg):
                    rcopy(d, *ini(d, grp, c)).start()

    def iny(d, c):
        return ys.at[c], yr.at[d - 2, c], iny_s.at[d - 2], iny_r.at[d - 2, c]

    def ter(d):
        if d == WEST:
            return terr.at[pl.ds(0, 8)], trx, ter_s.at[0], ter_r.at[0]
        return terr, tr_y, ter_s.at[1], ter_r.at[1]

    def uv(d):
        if d == WEST:
            return us_x, uh_x, uv_s.at[0], uv_r.at[0]
        return vs_y, vr_y, uv_s.at[1], uv_r.at[1]

    def stp(d, s):
        sems = stp_s.at[d], stp_r.at[d, lax.rem(s, 2)]
        if d < 2:
            row = LO if d == WEST else LO + bx - 1
            return pres.at[:, row, :], (pe_r, pw_r)[d].at[s], *sems
        return ps_y.at[s], pr_y.at[d - 2, s], *sems

    rows = lax.broadcasted_iota(jnp.int32, (bx, by), 0)
    lane = lax.broadcasted_iota(jnp.int32, (bx, by), 1)
    zero = jnp.zeros((bx, by), jnp.float32)

    def slab(k):
        return pl.ds(pl.multiple_of(k * bx, bx), bx)

    zrow = jnp.zeros((8, by), jnp.float32)

    def clear(k, carry):
        pres[k, pl.ds(0, 8), :] = zrow
        return carry

    lax.fori_loop(0, nz, clear, 0, unroll=8)

    for d in range(4):

        @pl.when(jnp.logical_not(has[opp[d]]))
        def _(d=d):
            if d == WEST:
                pe_r[...] = jnp.zeros(pe_r.shape, jnp.float32)
                uh_x[...] = jnp.zeros(uh_x.shape, jnp.float32)
                trx[...] = jnp.full(trx.shape, DRY, jnp.int32)
            if d == EAST:
                pw_r[...] = jnp.zeros(pw_r.shape, jnp.float32)
            if d < 2:
                at = pl.ds(LO + bx if d == WEST else 0, 8)

                def blank(k, carry):
                    for f in range(4):
                        raw[f, k, at, :] = zrow
                    return carry

                lax.fori_loop(0, nz, blank, 0, unroll=4)
            else:
                yr[d - 2] = jnp.zeros(yr.shape[1:], jnp.float32)
                pr_y[d - 2] = jnp.zeros(pr_y.shape[1:], jnp.float32)
            if d == SOUTH:
                tr_y[...] = jnp.full(tr_y.shape, DRY, jnp.int32)
                vr_y[...] = jnp.zeros(vr_y.shape, jnp.float32)

    small[0].wait()
    loads[0].wait()
    loads[1].wait()
    pl.semaphore_wait(barrier, sum(h.astype(jnp.int32) for h in has) + int(relay))
    start(WEST, ter(WEST))
    start(SOUTH, ter(SOUTH))
    for d in (WEST, EAST):
        start(d, *[ini(d, 0, c) for c in range(nkg)])
    loads[2].wait()
    loads[3].wait()
    if relay:
        for d, at in ((EAST, 1), (WEST, 2)):

            @pl.when(gx == at)
            def _(d=d):
                for grp in (1, 2):
                    rcopy_to(lax.rem(gx + 2, 4), *to_relay(d, grp)).start()

    start_direct(1)

    for c in small[1:]:
        c.wait()

    def pack(kg, carry):
        for f in range(4):
            acc = zero
            for kk in range(GROUP):
                x = raw[f, kg * GROUP + kk, pl.ds(LO, bx), :]
                acc = jnp.where((lane >> 3) == kk, pltpu.roll(x, 8 * kk + 3, 1), acc)
            ys[kg, f] = acc
        start(SOUTH, iny(SOUTH, kg))
        start(NORTH, iny(NORTH, kg))
        return carry

    lax.fori_loop(0, nkg, pack, 0)

    sq_r = lax.broadcasted_iota(jnp.int32, (by, by), 0)
    sq_c = lax.broadcasted_iota(jnp.int32, (by, by), 1)
    part = sq_r & 7
    far = jnp.where(part < 3, part - 3, jnp.where(part < 6, by - 3 + part, 8 * by))
    for src, at in ((sq_r, 0), (far, 2 * by)):
        for n in range(4):
            w = weights(src - sq_c - n // 2, (CENT, UPW)[n % 2])
            mat[pl.ds(at, by), pl.ds(n * by, by)] = w
            mat[pl.ds(at + by, by), pl.ds(n * by, by)] = w
        w = weights(src - sq_c - 1, {0: 1.0})
        mat_c[pl.ds(at, by), :] = w
        mat_c[pl.ds(at + by, by), :] = w

    def relax_of(ci, rj):
        best = None
        for n, dist in enumerate(
            (ci, (nx_dev * bx - 1.0) - ci, rj, (ny_dev * by - 1.0) - rj)
        ):
            width = jnp.full(ci.shape, zone[n], jnp.int32).astype(jnp.float32)
            ramp = jnp.maximum(width - dist, 0.0) / width
            best = ramp if best is None else jnp.maximum(best, ramp)
        return RELAX * best

    start_x = gx * bx
    start_y = gy * by
    ci = (rows + start_x).astype(jnp.float32)
    rj = (lane + start_y).astype(jnp.float32)
    relax = relax_of(ci, rj)
    keep = 1.0 - relax
    keep_out[...] = keep
    relax_hx = relax_of(
        (jnp.zeros((8, by), jnp.int32) + (start_x + bx)).astype(jnp.float32), rj[:8]
    )
    relax_hy = relax_of(ci, (jnp.zeros((bx, by), jnp.int32) + (start_y + by)).astype(jnp.float32))

    t0 = terr[...]

    def coeff(k, carry):
        c_prev, vrow = carry
        wet = t0 <= k
        gk = (ZC * ZC) * g[k]
        ga = (ZC * ZC) * jnp.where(k + 1 < nz, g[jnp.minimum(k + 1, nz - 1)], 0.0)
        inv = jnp.where(wet, 1.0 / (1.0 + ((ga + gk) - gk * c_prev)), 0.0)
        c_new = ga * inv
        wi[slab(k), :] = inv
        li[slab(k), :] = gk * inv
        cc[slab(k), :] = c_new
        ub_x[pl.ds(k, 1), :] = jnp.full((1, by), prof[0, k], jnp.float32)
        gh_x[pl.ds(k, 1), :] = jnp.full((1, by), g[k] * (HC * HC), jnp.float32)
        vrow = jnp.where((lane >> 1) == k, prof[1, k], vrow)
        return c_new, vrow

    _, vb_y = lax.fori_loop(0, nz, coeff, (zero, zero))

    sub8 = lax.broadcasted_iota(jnp.int32, (8, by), 0)
    scale = ADV / 60.0

    def along_y(kg, carry):
        wait_recv(SOUTH, iny(SOUTH, kg))
        wait_recv(NORTH, iny(NORTH, kg))
        for f in (FV, FU, FP, FW):
            halo = split(
                jnp.where((lane & 7) < 3, yr[NORTH - 2, kg, f], yr[SOUTH - 2, kg, f])
            )
            for kk in range(GROUP):
                at = pl.ds(kk * bx, bx)
                hi, lo = split(raw[f, kg * GROUP + kk, pl.ds(LO, bx), :])
                lhs[at, pl.ds(0, by)] = hi
                lhs[at, pl.ds(by, by)] = lo
                mine = (lane >> 3) == kk
                for n in range(2):
                    lhs[at, pl.ds((2 + n) * by, by)] = jnp.where(mine, halo[n], 0.0).astype(
                        jnp.bfloat16
                    )
            if f == FV:
                c_next[...] = scale * jnp.dot(
                    lhs[...], mat_c[...], preferred_element_type=jnp.float32
                )
            prod[...] = jnp.dot(lhs[...], mat[...], preferred_element_type=jnp.float32)
            for kk in range(GROUP):
                at = pl.ds(kk * bx, bx)
                k = kg * GROUP + kk
                c0 = raw[FV, k, pl.ds(LO, bx), :] * scale
                c1 = c_next[at, :]
                low = c0 * prod[at, pl.ds(0, by)] - jnp.abs(c0) * prod[at, pl.ds(by, by)]
                high = c1 * prod[at, pl.ds(2 * by, by)] - jnp.abs(c1) * prod[at, pl.ds(3 * by, by)]
                tend[f, slab(k), :] = raw[f, k, pl.ds(LO, bx), :] - (high - low)
        return carry

    lax.fori_loop(0, nkg, along_y, 0)

    forward(1)
    start_direct(2)

    wait_recv(WEST, ter(WEST))
    wait_recv(SOUTH, ter(SOUTH))
    t_east = jnp.broadcast_to(trx[0:1, :], (8, by))
    for k in range(0, nz, 8):
        wet_x[pl.ds(k, 8), :] = jnp.where(t_east <= sub8 + k, 1.0, 0.0)
    t_north = jnp.broadcast_to(tr_y[:, 0:1], (bx, by))
    wet_y = jnp.where(t_north <= (lane >> 1), 1.0, 0.0)


    def along_x(k, fields):
        n = bx + 8
        c = raw[FU, k, pl.ds(LO, n), :] * scale
        wet = t0 <= k
        res = []
        for f in fields:
            sh = [raw[f, k, pl.ds(LO + o, n), :] for o in (-3, -2, -1, 0, 1, 2)]
            flux = stencil(c, *sh)
            nxt = pltpu.roll(flux, n - 1, 0)[:bx]
            res.append(jnp.where(wet, tend[f, slab(k), :] - (nxt - flux[:bx]), 0.0))
        return res

    def wait_ini(grp, c):
        for d in (WEST, EAST):
            wait_recv(d, ini(d, grp, c))

    def first(k, acc):
        u, p = along_x(k, (FU, FP))
        p = HC * p
        u_out[k] = u
        pres[k, pl.ds(LO, bx), :] = p
        return jnp.where((lane >> 1) == k, pltpu.roll(p, 2 * k + 1, 1), acc)

    acc = zero
    for c in range(nkg):
        wait_ini(0, c)
        acc = lax.fori_loop(c * GROUP, (c + 1) * GROUP, first, acc, unroll=4)
    for n in range(0, nz, 8):
        us_x[pl.ds(n, 8), :] = u_out[pl.ds(n, 8), 0, :]
    start(WEST, stp(WEST, 0), uv(WEST))
    start(EAST, stp(EAST, 0))
    ps_y[0] = acc
    start(SOUTH, stp(SOUTH, 0))
    start(NORTH, stp(NORTH, 0))

    forward(2)

    def inner(k0, n, masked):
        stores = []
        for i in range(n):
            k = k0 + i
            p0 = pres[k, pl.ds(LO, bx), :]
            pm = pres[k, pl.ds(LO - 1, bx), :]
            un = u_out[k] - (p0 - pm)
            vn = v_out[k] - (p0 - jnp.where(lane == 0, 0.0, pltpu.roll(p0, 1, 1)))
            if masked:
                wet = t0 <= k
                un = jnp.where(wet, un, 0.0)
                vn = jnp.where(wet, vn, 0.0)
            un1 = jnp.where(rows == bx - 1, 0.0, pltpu.roll(un, bx - 1, 0))
            vn1 = jnp.where(lane == by - 1, 0.0, pltpu.roll(vn, by - 1, 1))
            q = p0 - (g[k] * (HC * HC)) * ((un1 - un) + (vn1 - vn))
            ur = keep * un + relax * prof[0, k]
            vr = keep * vn + relax * prof[1, k]
            if masked:
                q = jnp.where(wet, q, 0.0)
                ur = jnp.where(wet, ur, 0.0)
                vr = jnp.where(wet, vr, 0.0)
            stores.append((k, q, ur, vr))
        for k, q, ur, vr in stores:
            q_buf[slab(k), :] = q
            u_out[k] = ur
            v_out[k] = vr

    def second(k, acc):
        (v,) = along_x(k, (FV,))
        v_out[k] = v
        return jnp.where((lane >> 1) == k, pltpu.roll(v, 2 * k + 1, 1), acc)

    def third(k, carry):
        wsc[slab(k), :] = HC * along_x(k, (FW,))[0]
        return carry

    acc = zero
    for c in range(nkg):
        wait_ini(1, c)
        acc = lax.fori_loop(c * GROUP, (c + 1) * GROUP, second, acc, unroll=4)
        if c == 0:
            inner(0, TERRAIN_MAX, True)
            inner(TERRAIN_MAX, GROUP - TERRAIN_MAX, False)
        else:
            inner(c * GROUP, GROUP, False)
    vs_y[...] = acc
    start(SOUTH, uv(SOUTH))

    for c in range(nkg):
        wait_ini(2, c)
        lax.fori_loop(c * GROUP, (c + 1) * GROUP, third, 0, unroll=4)

    wait_recv(WEST, uv(WEST))
    wait_recv(SOUTH, uv(SOUTH))
    vh0 = pltpu.roll(vr_y[...], by - 1, 1)
    even = (lane & 1) == 0
    edge = jnp.logical_or(lane == 0, lane == by - 1)
    keep_w = jnp.broadcast_to(keep[0:1], (8, by))
    wet_lo = jnp.broadcast_to(t0[0:1], (8, by)) <= sub8
    wet_hi = jnp.broadcast_to(t0[bx - 1 : bx], (8, by)) <= sub8

    def edges_y(halo):
        for k in range(nz):
            add = jnp.where(edge, pltpu.roll(halo, by - 1 - 2 * k, 1), 0.0)
            if k < TERRAIN_MAX:
                add = jnp.where(t0 <= k, add, 0.0)
            q_buf[slab(k), :] = q_buf[slab(k), :] + (g[k] * (HC * HC)) * add
            v_out[k] = v_out[k] + jnp.where(lane == 0, keep * add, 0.0)

    wide = 8

    def over(body, *args):
        body(0, TERRAIN_MAX, *args, True)

        def step(n, carry):
            body(TERRAIN_MAX + n * wide, wide, *args, False)
            return carry

        lax.fori_loop(0, (nz - TERRAIN_MAX) // wide, step, 0)

    def halos(s, vh):
        wait_recv(SOUTH, stp(SOUTH, s))
        wait_recv(NORTH, stp(NORTH, s))
        vn_h = wet_y * (vh - (pltpu.roll(pr_y[SOUTH - 2, s], by - 1, 1) - ps_y[s]))
        vh_next = vn_h - relax_hy * (vn_h - wet_y * vb_y)
        halo = jnp.where(even, -vn_h, pltpu.roll(pr_y[NORTH - 2, s], 1, 1))
        edges_y(halo)
        for d in range(4):
            wait_send(d, stp(d, s))

        for d in (WEST, EAST):
            wait_recv(d, stp(d, s))
        for n in range(0, nz, 8):
            at = pl.ds(n, 8)
            gh = gh_x[at, :]
            pw = pw_r[s, at, :]
            if n < TERRAIN_MAX:
                pw = jnp.where(wet_lo, pw, 0.0)
            first_row = pl.ds(n * bx, 8, stride=bx)
            last_row = pl.ds(n * bx + bx - 1, 8, stride=bx)
            q_buf[first_row, :] = q_buf[first_row, :] + gh * pw
            wet = wet_x[at, :]
            un = wet * (uh_x[at, :] - (pe_r[s, at, :] - pres[pl.ds(n, 8), LO + bx - 1, :]))
            uh_x[at, :] = un
            if n < TERRAIN_MAX:
                un = jnp.where(wet_hi, un, 0.0)
            q_buf[last_row, :] = q_buf[last_row, :] - gh * un

        return vh_next

    def late(s):
        for n in range(0, nz, 8):
            at = pl.ds(n, 8)
            pw = pw_r[s, at, :]
            if n < TERRAIN_MAX:
                pw = jnp.where(wet_lo, pw, 0.0)
            u_out[at, 0, :] = u_out[at, 0, :] + keep_w * pw
            un = uh_x[at, :]
            uh_x[at, :] = un - relax_hx * (un - wet_x[at, :] * ub_x[at, :])

    def substep(s, vh):
        vh_next = halos(s, vh)
        q_prev = q_buf[slab(0), :]
        x = zero
        for k in range(nz):
            at = slab(k)
            q = q_buf[slab(k + 1), :] if k < nz - 1 else zero
            x = wi[at, :] * (wsc[at, :] - ZC * (q - q_prev)) + li[at, :] * x
            if k < nz - 1:
                d_buf[at, :] = x
            q_prev = q

        for k in range(nz - 1, -1, -1):
            below = zero
            if k > 0:
                below = d_buf[slab(k - 1), :] + cc[slab(k - 1), :] * x
            pres[k, pl.ds(LO, bx), :] = (q_buf[slab(k), :] - (g[k] * ZC) * (x - below)) * keep
            wsc[slab(k), :] = x * keep
            x = below

        start(WEST, stp(WEST, s + 1))
        start(EAST, stp(EAST, s + 1))

        late(s)
        acc = zero
        for k in range(nz):
            x = pltpu.roll(pres[k, pl.ds(LO, bx), :], 2 * k + 1, 1)
            acc = jnp.where((lane >> 1) == k, x, acc)
        ps_y[s + 1] = acc
        start(SOUTH, stp(SOUTH, s + 1))
        start(NORTH, stp(NORTH, s + 1))
        over(inner)
        return vh_next

    vh = lax.fori_loop(0, SUB - 1, substep, vh0)
    halos(SUB - 1, vh)
    late(SUB - 1)

    for d in (WEST, EAST):
        own = pl.ds(LO if d == WEST else LO + bx - 3, 3)
        far = pl.ds(LO + bx if d == WEST else LO - 3, 3)
        sent = raw.at[:, :, own, :], raw.at[:, :, far, :], ini_s.at[d], ini_r.at[d, 0, 0]
        wait_send(d, sent)

    if relay:

        @pl.when(jnp.logical_not(inner_x))
        def _():
            src = hop.at[:, :, pl.ds(0, 3), :]
            dst = raw.at[pl.ds(2, 2), :, pl.ds(LO - 3, 3), :]
            rcopy_to(lax.rem(gx + 2, 4), src, dst, fwd_s.at[0], ini_r.at[0, 0, 0]).wait_send()

    for d in (SOUTH, NORTH):
        wait_send(d, (ys, yr.at[d - 2], iny_s.at[d - 2], iny_r.at[d - 2, 0]))
    for d in (WEST, SOUTH):
        wait_send(d, ter(d), uv(d))


def last(
    nz, u, v, wsc, q, li, wi, cc, keep_ref, gh, u_out, v_out, w_out, p_out, w_buf, p_buf, d_buf, sems
):
    bx, by = keep_ref.shape
    copies = [
        pltpu.make_async_copy(u, u_out, sems.at[0]),
        pltpu.make_async_copy(v, v_out, sems.at[1]),
    ]
    for c in copies:
        c.start()
    keep = keep_ref[...]
    out = keep * (1.0 / HC)

    def slab(k):
        return pl.ds(k * bx, bx)

    zero = jnp.zeros((bx, by), jnp.float32)
    q_prev = q[slab(0), :]
    x = zero
    for k in range(nz):
        at = slab(k)
        q_next = q[slab(k + 1), :] if k < nz - 1 else zero
        x = wi[at, :] * (wsc[at, :] - ZC * (q_next - q_prev)) + li[at, :] * x
        if k < nz - 1:
            d_buf[at, :] = x
        q_prev = q_next

    half = nz // 2
    for h in (1, 0):
        for k in range((h + 1) * half - 1, h * half - 1, -1):
            below = zero
            if k > 0:
                below = d_buf[slab(k - 1), :] + cc[slab(k - 1), :] * x
            gz = gh[pl.ds(k, 1), :] * (ZC / (HC * HC))
            p_buf[k] = (q[slab(k), :] - gz * (x - below)) * out
            w_buf[k] = x * out
            x = below
        part = pl.ds(h * half, half)
        for n, (src, dst) in enumerate(((w_buf, w_out), (p_buf, p_out))):
            c = pltpu.make_async_copy(src.at[part], dst.at[part], sems.at[2 + 2 * h + n])
            c.start()
            copies.append(c)
    for c in copies:
        c.wait()


def solution(mesh):
    cnt = (mesh.shape["gx"], mesh.shape["gy"])

    def on_device(u, v, w, p, terr, zone, g, prof):
        nz, bx, by = u.shape
        assert by == 128 and bx == 16 and 2 * nz == by
        f32 = jnp.float32
        vm = pltpu.VMEM
        dma = pltpu.SemaphoreType.DMA
        nkg = nz // GROUP
        lev = vm((nz * bx, by), f32)
        col = vm((nz, by), f32)
        plane = vm((bx, by), f32)
        plane_i = vm((bx, by), jnp.int32)
        scratch = [
            plane_i,
            pltpu.SMEM(zone.shape, jnp.int32),
            pltpu.SMEM(g.shape, f32),
            pltpu.SMEM(prof.shape, f32),
            vm((4, nz, ROWS, by), f32),
            vm((4, nz * bx, by), f32),
            vm((nz, PEXT, by), f32),
            lev,
            vm((GROUP * bx, 4 * by), jnp.bfloat16),
            vm((4 * by, 4 * by), jnp.bfloat16),
            vm((4 * by, by), jnp.bfloat16),
            vm((GROUP * bx, 4 * by), f32),
            vm((GROUP * bx, by), f32),
            vm((nkg, 4, bx, by), f32),
            vm((2, nkg, 4, bx, by), f32),
            vm((8, by), jnp.int32),
            vm((bx, by), jnp.int32),
            vm((SUB, nz, by), f32),
            vm((SUB, nz, by), f32),
            vm((SUB, bx, by), f32),
            vm((2, SUB, bx, by), f32),
            col, col, plane, plane, col, col,
            dma((8,)),
            dma((2,)), dma((2, 3, nkg)),
            dma((2,)), dma((2, nkg)),
            dma((2,)), dma((2,)),
            dma((2,)), dma((2,)),
            dma((4,)), dma((4, 2)),
            vm((2, nz, 8, by), f32),
            dma((2,)), dma((1,)),
        ]
        vspec = pl.BlockSpec(memory_space=pltpu.VMEM)
        aspec = pl.BlockSpec(memory_space=pl.ANY)
        outs = pl.pallas_call(
            functools.partial(kernel, nz, bx, cnt),
            out_shape=[pltpu.VMEM((nz, bx, by), f32)] * 2
            + [pltpu.VMEM((nz * bx, by), f32)] * 5
            + [pltpu.VMEM((bx, by), f32), pltpu.VMEM((nz, by), f32)],
            in_specs=[pl.BlockSpec(memory_space=pltpu.HBM)] * 8,
            out_specs=[vspec] * 9,
            scratch_shapes=scratch,
            compiler_params=pltpu.CompilerParams(
                collective_id=0, has_side_effects=True, vmem_limit_bytes=VMEM_LIMIT
            ),
        )(u, v, w, p, terr, zone, g, prof)
        outs = [pltpu.with_memory_space_constraint(a, pltpu.VMEM) for a in outs]
        full = vm((nz, bx, by), f32)
        return pl.pallas_call(
            functools.partial(last, nz),
            out_shape=[jax.ShapeDtypeStruct((nz, bx, by), f32)] * 4,
            in_specs=[vspec] * 9,
            out_specs=[aspec] * 4,
            scratch_shapes=[full, full, lev, dma((6,))],
            compiler_params=pltpu.CompilerParams(vmem_limit_bytes=VMEM_LIMIT),
        )(*outs)

    field = P(None, "gx", "gy")
    return jax.shard_map(
        on_device,
        mesh=mesh,
        in_specs=(field, field, field, field, P("gx", "gy"), P(), P(), P()),
        out_specs=(field,) * 4,
        check_vma=False,
    )
```

```python
import functools

import jax
import jax.numpy as jnp
from jax import lax
from jax.experimental import pallas as pl
from jax.experimental.pallas import tpu as pltpu
from jax.sharding import PartitionSpec as P

SUB = 6
ADV = 0.3
HC = 0.4
ZC = 1.0
RELAX = 0.5
TERRAIN_MAX = 8
DRY = 1 << 20
WEST, EAST, SOUTH, NORTH = 0, 1, 2, 3
FU, FP, FV, FW = 0, 1, 2, 3
LO = 8
ROWS = 40
PEXT = 24
GROUP = 16
VMEM_LIMIT = 59 << 20
CENT = {-3: 1.0, -2: -8.0, -1: 37.0, 0: 37.0, 1: -8.0, 2: 1.0}
UPW = {-3: -1.0, -2: 5.0, -1: -10.0, 0: 10.0, 1: -5.0, 2: 1.0}


def stencil(c, m3, m2, m1, f0, e1, e2):
    centered = 37.0 * (f0 + m1) - 8.0 * (e1 + m2) + (e2 + m3)
    upwind = 10.0 * (f0 - m1) - 5.0 * (e1 - m2) + (e2 - m3)
    return c * centered - jnp.abs(c) * upwind


def weights(dist, table):
    out = jnp.zeros(dist.shape, jnp.float32)
    for off, value in table.items():
        out = jnp.where(dist == off, value, out)
    return out.astype(jnp.bfloat16)


def split(x):
    hi = x.astype(jnp.bfloat16)
    return hi, (x - hi.astype(jnp.float32)).astype(jnp.bfloat16)


def kernel(
    nz,
    bx,
    cnt,
    u_in,
    v_in,
    w_in,
    p_in,
    terr_in,
    zone_in,
    g_in,
    prof_in,
    u_out,
    v_out,
    wsc,
    q_buf,
    li,
    wi,
    cc,
    keep_out,
    gh_x,
    terr,
    zone,
    g,
    prof,
    raw,
    tend,
    pres,
    d_buf,
    lhs,
    mat,
    mat_c,
    prod,
    c_next,
    ys,
    yr,
    trx,
    tr_y,
    pw_r,
    pe_r,
    ps_y,
    pr_y,
    us_x,
    uh_x,
    vs_y,
    vr_y,
    ub_x,
    wet_x,
    in_s,
    ini_s,
    ini_r,
    iny_s,
    iny_r,
    ter_s,
    ter_r,
    uv_s,
    uv_r,
    stp_s,
    stp_r,
    hop,
    hop_r,
    fwd_s,
):
    by = 128
    nkg = nz // GROUP
    gx = lax.axis_index("gx")
    gy = lax.axis_index("gy")
    nx_dev, ny_dev = cnt
    has = (gx > 0, gx < nx_dev - 1, gy > 0, gy < ny_dev - 1)
    peer = ({"gx": gx - 1}, {"gx": gx + 1}, {"gy": gy - 1}, {"gy": gy + 1})
    opp = (EAST, WEST, NORTH, SOUTH)

    relay = nx_dev == 4
    inner_x = jnp.logical_or(gx == 1, gx == 2)

    barrier = pltpu.get_barrier_semaphore()

    def greet(dev):
        pl.semaphore_signal(barrier, inc=1, device_id=dev, device_id_type=pl.DeviceIdType.MESH)

    for d in range(4):

        @pl.when(has[d])
        def _(d=d):
            greet(peer[d])

    if relay:
        greet({"gx": lax.rem(gx + 2, 4)})

    loads = [
        pltpu.make_async_copy(src, raw.at[f, :, pl.ds(LO, bx), :], in_s.at[f // 2])
        for f, src in ((FU, u_in), (FP, p_in), (FV, v_in), (FW, w_in))
    ]
    small = [
        pltpu.make_async_copy(src, dst, in_s.at[2 + n])
        for n, (src, dst) in enumerate(
            ((terr_in, terr), (zone_in, zone), (g_in, g), (prof_in, prof))
        )
    ]
    for c in loads + small:
        c.start()

    def loaded(n):
        pair = raw.at[pl.ds(2 * n, 2), :, pl.ds(LO, bx), :]
        pltpu.make_async_copy(pair, pair, in_s.at[n]).wait()

    def rcopy(d, src, dst, ss, rs):
        return pltpu.make_async_remote_copy(
            src_ref=src,
            dst_ref=dst,
            send_sem=ss,
            recv_sem=rs,
            device_id=peer[d],
            device_id_type=pl.DeviceIdType.MESH,
        )

    def start(d, *copies):
        @pl.when(has[d])
        def _():
            for c in copies:
                rcopy(d, *c).start()

    def wait_send(d, *copies):
        @pl.when(has[d])
        def _():
            for c in copies:
                rcopy(d, *c).wait_send()

    def wait_recv(d, *copies):
        @pl.when(has[opp[d]])
        def _():
            for c in copies:
                rcopy(d, *c).wait_recv()

    blocks = (nkg, nkg // 2, nkg)

    def ini(d, grp, c=None):
        own = LO if d == WEST else LO + bx - 3
        far = LO + bx if d == WEST else LO - 3
        f = pl.ds(0, 2) if grp == 0 else grp + 1
        k = pl.ds(0, nz) if c is None else pl.ds(c * (nz // blocks[grp]), nz // blocks[grp])
        return (
            raw.at[f, k, pl.ds(own, 3), :],
            raw.at[f, k, pl.ds(far, 3), :],
            ini_s.at[d],
            ini_r.at[d, sum(blocks[:grp]) + (0 if c is None else c)],
        )

    def direct(d):
        if not relay:
            return has[d]
        return jnp.logical_and(has[d], gx != (2, 1)[d])

    def rcopy_to(dev, src, dst, ss, rs):
        return pltpu.make_async_remote_copy(
            src_ref=src,
            dst_ref=dst,
            send_sem=ss,
            recv_sem=rs,
            device_id={"gx": dev},
            device_id_type=pl.DeviceIdType.MESH,
        )

    def to_relay(d, grp):
        dst = hop.at[grp - 1, :, pl.ds(0, 3), :]
        return ini(d, grp)[0], dst, ini_s.at[d], hop_r.at[grp - 1]

    def from_relay(d, grp, c=None):
        k = pl.ds(0, nz) if c is None else pl.ds(c * (nz // blocks[grp]), nz // blocks[grp])
        _, dst, _, sem = ini(d, grp, c)
        return hop.at[grp - 1, k, pl.ds(0, 3), :], dst, fwd_s.at[0], sem

    def forward(grp):
        if relay:
            for d, at in ((EAST, 3), (WEST, 0)):

                @pl.when(gx == at)
                def _(d=d):
                    rcopy_to(lax.rem(gx + 2, 4), *to_relay(d, grp)).wait_recv()
                    for c in range(blocks[grp]):
                        rcopy_to((gx + 1, gx - 1)[d == EAST], *from_relay(d, grp, c)).start()

    def start_direct(grp):
        for d in (WEST, EAST):

            @pl.when(direct(d))
            def _(d=d):
                for c in range(blocks[grp]):
                    rcopy(d, *ini(d, grp, c)).start()

    def iny(d, c):
        return ys.at[c], yr.at[d - 2, c], iny_s.at[d - 2], iny_r.at[d - 2, c]

    def ter(d):
        if d == WEST:
            return terr.at[pl.ds(0, 8)], trx, ter_s.at[0], ter_r.at[0]
        return terr, tr_y, ter_s.at[1], ter_r.at[1]

    def uv(d):
        if d == WEST:
            return us_x, uh_x, uv_s.at[0], uv_r.at[0]
        return vs_y, vr_y, uv_s.at[1], uv_r.at[1]

    def stp(d, s):
        sems = stp_s.at[d], stp_r.at[d, lax.rem(s, 2)]
        if d < 2:
            row = LO if d == WEST else LO + bx - 1
            return pres.at[:, row, :], (pe_r, pw_r)[d].at[s], *sems
        return ps_y.at[s], pr_y.at[d - 2, s], *sems

    rows = lax.broadcasted_iota(jnp.int32, (bx, by), 0)
    lane = lax.broadcasted_iota(jnp.int32, (bx, by), 1)
    zero = jnp.zeros((bx, by), jnp.float32)

    def slab(k):
        return pl.ds(pl.multiple_of(k * bx, bx), bx)

    zrow = jnp.zeros((8, by), jnp.float32)

    def clear(k, carry):
        pres[k, pl.ds(0, 8), :] = zrow
        return carry

    lax.fori_loop(0, nz, clear, 0, unroll=8)

    for d in range(4):

        @pl.when(jnp.logical_not(has[opp[d]]))
        def _(d=d):
            if d == WEST:
                pe_r[...] = jnp.zeros(pe_r.shape, jnp.float32)
                uh_x[...] = jnp.zeros(uh_x.shape, jnp.float32)
                trx[...] = jnp.full(trx.shape, DRY, jnp.int32)
            if d == EAST:
                pw_r[...] = jnp.zeros(pw_r.shape, jnp.float32)
            if d < 2:
                at = pl.ds(LO + bx if d == WEST else 0, 8)

                def blank(k, carry):
                    for f in range(4):
                        raw[f, k, at, :] = zrow
                    return carry

                lax.fori_loop(0, nz, blank, 0, unroll=4)
            else:
                yr[d - 2] = jnp.zeros(yr.shape[1:], jnp.float32)
                pr_y[d - 2] = jnp.zeros(pr_y.shape[1:], jnp.float32)
            if d == SOUTH:
                tr_y[...] = jnp.full(tr_y.shape, DRY, jnp.int32)
                vr_y[...] = jnp.zeros(vr_y.shape, jnp.float32)

    small[0].wait()
    loaded(0)
    pl.semaphore_wait(barrier, sum(h.astype(jnp.int32) for h in has) + int(relay))
    start(WEST, ter(WEST))
    start(SOUTH, ter(SOUTH))
    for d in (WEST, EAST):
        start(d, *[ini(d, 0, c) for c in range(nkg)])
    loaded(1)
    if relay:
        for d, at in ((EAST, 1), (WEST, 2)):

            @pl.when(gx == at)
            def _(d=d):
                for grp in (1, 2):
                    rcopy_to(lax.rem(gx + 2, 4), *to_relay(d, grp)).start()

    start_direct(1)

    for c in small[1:]:
        c.wait()

    def pack(kg, carry):
        for f in range(4):
            acc = zero
            for kk in range(GROUP):
                x = raw[f, kg * GROUP + kk, pl.ds(LO, bx), :]
                acc = jnp.where((lane >> 3) == kk, pltpu.roll(x, 8 * kk + 3, 1), acc)
            ys[kg, f] = acc
        start(SOUTH, iny(SOUTH, kg))
        start(NORTH, iny(NORTH, kg))
        return carry

    lax.fori_loop(0, nkg, pack, 0)

    sq_r = lax.broadcasted_iota(jnp.int32, (by, by), 0)
    sq_c = lax.broadcasted_iota(jnp.int32, (by, by), 1)
    part = sq_r & 7
    far = jnp.where(part < 3, part - 3, jnp.where(part < 6, by - 3 + part, 8 * by))
    for src, at in ((sq_r, 0), (far, 2 * by)):
        for n in range(4):
            w = weights(src - sq_c - n // 2, (CENT, UPW)[n % 2])
            mat[pl.ds(at, by), pl.ds(n * by, by)] = w
            mat[pl.ds(at + by, by), pl.ds(n * by, by)] = w
        w = weights(src - sq_c - 1, {0: 1.0})
        mat_c[pl.ds(at, by), :] = w
        mat_c[pl.ds(at + by, by), :] = w

    def relax_of(ci, rj):
        best = None
        for n, dist in enumerate(
            (ci, (nx_dev * bx - 1.0) - ci, rj, (ny_dev * by - 1.0) - rj)
        ):
            width = jnp.full(ci.shape, zone[n], jnp.int32).astype(jnp.float32)
            ramp = jnp.maximum(width - dist, 0.0) / width
            best = ramp if best is None else jnp.maximum(best, ramp)
        return RELAX * best

    start_x = gx * bx
    start_y = gy * by
    ci = (rows + start_x).astype(jnp.float32)
    rj = (lane + start_y).astype(jnp.float32)
    relax = relax_of(ci, rj)
    keep = 1.0 - relax
    keep_out[...] = keep
    relax_hx = relax_of(
        (jnp.zeros((8, by), jnp.int32) + (start_x + bx)).astype(jnp.float32), rj[:8]
    )
    relax_hy = relax_of(ci, (jnp.zeros((bx, by), jnp.int32) + (start_y + by)).astype(jnp.float32))

    t0 = terr[...]

    def coeff(k, carry):
        c_prev, vrow = carry
        wet = t0 <= k
        gk = (ZC * ZC) * g[k]
        ga = (ZC * ZC) * jnp.where(k + 1 < nz, g[jnp.minimum(k + 1, nz - 1)], 0.0)
        inv = jnp.where(wet, 1.0 / (1.0 + ((ga + gk) - gk * c_prev)), 0.0)
        c_new = ga * inv
        wi[slab(k), :] = inv
        li[slab(k), :] = gk * inv
        cc[slab(k), :] = c_new
        ub_x[pl.ds(k, 1), :] = jnp.full((1, by), prof[0, k], jnp.float32)
        gh_x[pl.ds(k, 1), :] = jnp.full((1, by), g[k] * (HC * HC), jnp.float32)
        vrow = jnp.where((lane >> 1) == k, prof[1, k], vrow)
        return c_new, vrow

    _, vb_y = lax.fori_loop(0, nz, coeff, (zero, zero))

    sub8 = lax.broadcasted_iota(jnp.int32, (8, by), 0)
    scale = ADV / 60.0

    def along_y(kg, carry):
        wait_recv(SOUTH, iny(SOUTH, kg))
        wait_recv(NORTH, iny(NORTH, kg))
        for f in (FV, FU, FP, FW):
            halo = split(
                jnp.where((lane & 7) < 3, yr[NORTH - 2, kg, f], yr[SOUTH - 2, kg, f])
            )
            for kk in range(GROUP):
                at = pl.ds(kk * bx, bx)
                hi, lo = split(raw[f, kg * GROUP + kk, pl.ds(LO, bx), :])
                lhs[at, pl.ds(0, by)] = hi
                lhs[at, pl.ds(by, by)] = lo
                mine = (lane >> 3) == kk
                for n in range(2):
                    lhs[at, pl.ds((2 + n) * by, by)] = jnp.where(mine, halo[n], 0.0).astype(
                        jnp.bfloat16
                    )
            if f == FV:
                c_next[...] = scale * jnp.dot(
                    lhs[...], mat_c[...], preferred_element_type=jnp.float32
                )
            prod[...] = jnp.dot(lhs[...], mat[...], preferred_element_type=jnp.float32)
            for kk in range(GROUP):
                at = pl.ds(kk * bx, bx)
                k = kg * GROUP + kk
                c0 = raw[FV, k, pl.ds(LO, bx), :] * scale
                c1 = c_next[at, :]
                low = c0 * prod[at, pl.ds(0, by)] - jnp.abs(c0) * prod[at, pl.ds(by, by)]
                high = c1 * prod[at, pl.ds(2 * by, by)] - jnp.abs(c1) * prod[at, pl.ds(3 * by, by)]
                tend[f, slab(k), :] = raw[f, k, pl.ds(LO, bx), :] - (high - low)
        return carry

    lax.fori_loop(0, nkg, along_y, 0)

    forward(1)
    start_direct(2)

    wait_recv(WEST, ter(WEST))
    wait_recv(SOUTH, ter(SOUTH))
    t_east = jnp.broadcast_to(trx[0:1, :], (8, by))
    for k in range(0, nz, 8):
        wet_x[pl.ds(k, 8), :] = jnp.where(t_east <= sub8 + k, 1.0, 0.0)
    t_north = jnp.broadcast_to(tr_y[:, 0:1], (bx, by))
    wet_y = jnp.where(t_north <= (lane >> 1), 1.0, 0.0)


    def along_x(k, fields):
        n = bx + 8
        c = raw[FU, k, pl.ds(LO, n), :] * scale
        wet = t0 <= k
        res = []
        for f in fields:
            sh = [raw[f, k, pl.ds(LO + o, n), :] for o in (-3, -2, -1, 0, 1, 2)]
            flux = stencil(c, *sh)
            nxt = pltpu.roll(flux, n - 1, 0)[:bx]
            res.append(jnp.where(wet, tend[f, slab(k), :] - (nxt - flux[:bx]), 0.0))
        return res

    def wait_ini(grp, c):
        for d in (WEST, EAST):
            wait_recv(d, ini(d, grp, c))

    def first(k, acc):
        u, p = along_x(k, (FU, FP))
        p = HC * p
        u_out[k] = u
        pres[k, pl.ds(LO, bx), :] = p
        return jnp.where((lane >> 1) == k, pltpu.roll(p, 2 * k + 1, 1), acc)

    acc = zero
    for c in range(nkg):
        wait_ini(0, c)
        acc = lax.fori_loop(c * GROUP, (c + 1) * GROUP, first, acc, unroll=4)
    for n in range(0, nz, 8):
        us_x[pl.ds(n, 8), :] = u_out[pl.ds(n, 8), 0, :]
    start(WEST, stp(WEST, 0), uv(WEST))
    start(EAST, stp(EAST, 0))
    ps_y[0] = acc
    start(SOUTH, stp(SOUTH, 0))
    start(NORTH, stp(NORTH, 0))

    forward(2)

    def inner(k0, n, masked):
        stores = []
        for i in range(n):
            k = k0 + i
            p0 = pres[k, pl.ds(LO, bx), :]
            pm = pres[k, pl.ds(LO - 1, bx), :]
            un = u_out[k] - (p0 - pm)
            vn = v_out[k] - (p0 - jnp.where(lane == 0, 0.0, pltpu.roll(p0, 1, 1)))
            if masked:
                wet = t0 <= k
                un = jnp.where(wet, un, 0.0)
                vn = jnp.where(wet, vn, 0.0)
            un1 = jnp.where(rows == bx - 1, 0.0, pltpu.roll(un, bx - 1, 0))
            vn1 = jnp.where(lane == by - 1, 0.0, pltpu.roll(vn, by - 1, 1))
            q = p0 - (g[k] * (HC * HC)) * ((un1 - un) + (vn1 - vn))
            ur = keep * un + relax * prof[0, k]
            vr = keep * vn + relax * prof[1, k]
            if masked:
                q = jnp.where(wet, q, 0.0)
                ur = jnp.where(wet, ur, 0.0)
                vr = jnp.where(wet, vr, 0.0)
            stores.append((k, q, ur, vr))
        for k, q, ur, vr in stores:
            q_buf[slab(k), :] = q
            u_out[k] = ur
            v_out[k] = vr

    def second(k, acc):
        (v,) = along_x(k, (FV,))
        v_out[k] = v
        return jnp.where((lane >> 1) == k, pltpu.roll(v, 2 * k + 1, 1), acc)

    def third(k, carry):
        wsc[slab(k), :] = HC * along_x(k, (FW,))[0]
        return carry

    acc = zero
    for c in range(nkg):
        if c % 2 == 0:
            wait_ini(1, c // 2)
        acc = lax.fori_loop(c * GROUP, (c + 1) * GROUP, second, acc, unroll=4)
        if c == 0:
            inner(0, TERRAIN_MAX, True)
            inner(TERRAIN_MAX, GROUP - TERRAIN_MAX, False)
        else:
            inner(c * GROUP, GROUP, False)
    vs_y[...] = acc
    start(SOUTH, uv(SOUTH))

    for c in range(nkg):
        wait_ini(2, c)
        lax.fori_loop(c * GROUP, (c + 1) * GROUP, third, 0, unroll=4)

    wait_recv(WEST, uv(WEST))
    wait_recv(SOUTH, uv(SOUTH))
    vh0 = pltpu.roll(vr_y[...], by - 1, 1)
    even = (lane & 1) == 0
    edge = jnp.logical_or(lane == 0, lane == by - 1)
    keep_w = jnp.broadcast_to(keep[0:1], (8, by))
    wet_lo = jnp.broadcast_to(t0[0:1], (8, by)) <= sub8
    wet_hi = jnp.broadcast_to(t0[bx - 1 : bx], (8, by)) <= sub8

    def edges_y(halo):
        for k in range(nz):
            add = jnp.where(edge, pltpu.roll(halo, by - 1 - 2 * k, 1), 0.0)
            if k < TERRAIN_MAX:
                add = jnp.where(t0 <= k, add, 0.0)
            q_buf[slab(k), :] = q_buf[slab(k), :] + (g[k] * (HC * HC)) * add
            v_out[k] = v_out[k] + jnp.where(lane == 0, keep * add, 0.0)

    wide = 8

    def over(body, *args):
        body(0, TERRAIN_MAX, *args, True)

        def step(n, carry):
            body(TERRAIN_MAX + n * wide, wide, *args, False)
            return carry

        lax.fori_loop(0, (nz - TERRAIN_MAX) // wide, step, 0)

    def halos(s, vh):
        wait_recv(SOUTH, stp(SOUTH, s))
        wait_recv(NORTH, stp(NORTH, s))
        vn_h = wet_y * (vh - (pltpu.roll(pr_y[SOUTH - 2, s], by - 1, 1) - ps_y[s]))
        vh_next = vn_h - relax_hy * (vn_h - wet_y * vb_y)
        halo = jnp.where(even, -vn_h, pltpu.roll(pr_y[NORTH - 2, s], 1, 1))
        edges_y(halo)
        for d in range(4):
            wait_send(d, stp(d, s))

        for d in (WEST, EAST):
            wait_recv(d, stp(d, s))
        for n in range(0, nz, 8):
            at = pl.ds(n, 8)
            gh = gh_x[at, :]
            pw = pw_r[s, at, :]
            if n < TERRAIN_MAX:
                pw = jnp.where(wet_lo, pw, 0.0)
            first_row = pl.ds(n * bx, 8, stride=bx)
            last_row = pl.ds(n * bx + bx - 1, 8, stride=bx)
            q_buf[first_row, :] = q_buf[first_row, :] + gh * pw
            wet = wet_x[at, :]
            un = wet * (uh_x[at, :] - (pe_r[s, at, :] - pres[pl.ds(n, 8), LO + bx - 1, :]))
            uh_x[at, :] = un
            if n < TERRAIN_MAX:
                un = jnp.where(wet_hi, un, 0.0)
            q_buf[last_row, :] = q_buf[last_row, :] - gh * un

        return vh_next

    def late(s):
        for n in range(0, nz, 8):
            at = pl.ds(n, 8)
            pw = pw_r[s, at, :]
            if n < TERRAIN_MAX:
                pw = jnp.where(wet_lo, pw, 0.0)
            u_out[at, 0, :] = u_out[at, 0, :] + keep_w * pw
            un = uh_x[at, :]
            uh_x[at, :] = un - relax_hx * (un - wet_x[at, :] * ub_x[at, :])

    def substep(s, vh):
        vh_next = halos(s, vh)
        q_prev = q_buf[slab(0), :]
        x = zero
        for k in range(nz):
            at = slab(k)
            q = q_buf[slab(k + 1), :] if k < nz - 1 else zero
            x = wi[at, :] * (wsc[at, :] - ZC * (q - q_prev)) + li[at, :] * x
            if k < nz - 1:
                d_buf[at, :] = x
            q_prev = q

        for k in range(nz - 1, -1, -1):
            below = zero
            if k > 0:
                below = d_buf[slab(k - 1), :] + cc[slab(k - 1), :] * x
            pres[k, pl.ds(LO, bx), :] = (q_buf[slab(k), :] - (g[k] * ZC) * (x - below)) * keep
            wsc[slab(k), :] = x * keep
            x = below

        start(WEST, stp(WEST, s + 1))
        start(EAST, stp(EAST, s + 1))

        late(s)
        acc = zero
        for k in range(nz):
            x = pltpu.roll(pres[k, pl.ds(LO, bx), :], 2 * k + 1, 1)
            acc = jnp.where((lane >> 1) == k, x, acc)
        ps_y[s + 1] = acc
        start(SOUTH, stp(SOUTH, s + 1))
        start(NORTH, stp(NORTH, s + 1))
        over(inner)
        return vh_next

    vh = lax.fori_loop(0, SUB - 1, substep, vh0)
    halos(SUB - 1, vh)
    late(SUB - 1)

    for d in (WEST, EAST):
        own = pl.ds(LO if d == WEST else LO + bx - 3, 3)
        far = pl.ds(LO + bx if d == WEST else LO - 3, 3)
        sent = raw.at[:, :, own, :], raw.at[:, :, far, :], ini_s.at[d], ini_r.at[d, 0]
        wait_send(d, sent)

    if relay:

        @pl.when(jnp.logical_not(inner_x))
        def _():
            src = hop.at[:, :, pl.ds(0, 3), :]
            dst = raw.at[pl.ds(2, 2), :, pl.ds(LO - 3, 3), :]
            rcopy_to(lax.rem(gx + 2, 4), src, dst, fwd_s.at[0], ini_r.at[0, 0]).wait_send()

    for d in (SOUTH, NORTH):
        wait_send(d, (ys, yr.at[d - 2], iny_s.at[d - 2], iny_r.at[d - 2, 0]))
    for d in (WEST, SOUTH):
        wait_send(d, ter(d), uv(d))


def last(
    nz, u, v, wsc, q, li, wi, cc, keep_ref, gh, u_out, v_out, w_out, p_out, w_buf, p_buf, d_buf, sems
):
    bx, by = keep_ref.shape
    copies = [
        pltpu.make_async_copy(u, u_out, sems.at[0]),
        pltpu.make_async_copy(v, v_out, sems.at[1]),
    ]
    for c in copies:
        c.start()
    keep = keep_ref[...]
    out = keep * (1.0 / HC)

    def slab(k):
        return pl.ds(k * bx, bx)

    zero = jnp.zeros((bx, by), jnp.float32)
    q_prev = q[slab(0), :]
    x = zero
    for k in range(nz):
        at = slab(k)
        q_next = q[slab(k + 1), :] if k < nz - 1 else zero
        x = wi[at, :] * (wsc[at, :] - ZC * (q_next - q_prev)) + li[at, :] * x
        if k < nz - 1:
            d_buf[at, :] = x
        q_prev = q_next

    half = nz // 2
    for h in (1, 0):
        for k in range((h + 1) * half - 1, h * half - 1, -1):
            below = zero
            if k > 0:
                below = d_buf[slab(k - 1), :] + cc[slab(k - 1), :] * x
            gz = gh[pl.ds(k, 1), :] * (ZC / (HC * HC))
            p_buf[k] = (q[slab(k), :] - gz * (x - below)) * out
            w_buf[k] = x * out
            x = below
        part = pl.ds(h * half, half)
        for n, (src, dst) in enumerate(((w_buf, w_out), (p_buf, p_out))):
            c = pltpu.make_async_copy(src.at[part], dst.at[part], sems.at[2 + 2 * h + n])
            c.start()
            copies.append(c)
    for c in copies:
        c.wait()


def solution(mesh):
    cnt = (mesh.shape["gx"], mesh.shape["gy"])

    def on_device(u, v, w, p, terr, zone, g, prof):
        nz, bx, by = u.shape
        assert by == 128 and bx == 16 and 2 * nz == by
        f32 = jnp.float32
        vm = pltpu.VMEM
        dma = pltpu.SemaphoreType.DMA
        nkg = nz // GROUP
        lev = vm((nz * bx, by), f32)
        col = vm((nz, by), f32)
        plane = vm((bx, by), f32)
        plane_i = vm((bx, by), jnp.int32)
        scratch = [
            plane_i,
            pltpu.SMEM(zone.shape, jnp.int32),
            pltpu.SMEM(g.shape, f32),
            pltpu.SMEM(prof.shape, f32),
            vm((4, nz, ROWS, by), f32),
            vm((4, nz * bx, by), f32),
            vm((nz, PEXT, by), f32),
            lev,
            vm((GROUP * bx, 4 * by), jnp.bfloat16),
            vm((4 * by, 4 * by), jnp.bfloat16),
            vm((4 * by, by), jnp.bfloat16),
            vm((GROUP * bx, 4 * by), f32),
            vm((GROUP * bx, by), f32),
            vm((nkg, 4, bx, by), f32),
            vm((2, nkg, 4, bx, by), f32),
            vm((8, by), jnp.int32),
            vm((bx, by), jnp.int32),
            vm((SUB, nz, by), f32),
            vm((SUB, nz, by), f32),
            vm((SUB, bx, by), f32),
            vm((2, SUB, bx, by), f32),
            col, col, plane, plane, col, col,
            dma((6,)),
            dma((2,)), dma((2, 2 * nkg + nkg // 2)),
            dma((2,)), dma((2, nkg)),
            dma((2,)), dma((2,)),
            dma((2,)), dma((2,)),
            dma((4,)), dma((4, 2)),
            vm((2, nz, 8, by), f32),
            dma((2,)), dma((1,)),
        ]
        vspec = pl.BlockSpec(memory_space=pltpu.VMEM)
        aspec = pl.BlockSpec(memory_space=pl.ANY)
        outs = pl.pallas_call(
            functools.partial(kernel, nz, bx, cnt),
            out_shape=[pltpu.VMEM((nz, bx, by), f32)] * 2
            + [pltpu.VMEM((nz * bx, by), f32)] * 5
            + [pltpu.VMEM((bx, by), f32), pltpu.VMEM((nz, by), f32)],
            in_specs=[pl.BlockSpec(memory_space=pltpu.HBM)] * 8,
            out_specs=[vspec] * 9,
            scratch_shapes=scratch,
            compiler_params=pltpu.CompilerParams(
                collective_id=0, has_side_effects=True, vmem_limit_bytes=VMEM_LIMIT
            ),
        )(u, v, w, p, terr, zone, g, prof)
        outs = [pltpu.with_memory_space_constraint(a, pltpu.VMEM) for a in outs]
        full = vm((nz, bx, by), f32)
        return pl.pallas_call(
            functools.partial(last, nz),
            out_shape=[jax.ShapeDtypeStruct((nz, bx, by), f32)] * 4,
            in_specs=[vspec] * 9,
            out_specs=[aspec] * 4,
            scratch_shapes=[full, full, lev, dma((6,))],
            compiler_params=pltpu.CompilerParams(vmem_limit_bytes=VMEM_LIMIT),
        )(*outs)

    field = P(None, "gx", "gy")
    return jax.shard_map(
        on_device,
        mesh=mesh,
        in_specs=(field, field, field, field, P("gx", "gy"), P(), P(), P()),
        out_specs=(field,) * 4,
        check_vma=False,
    )
```
